32 devices in a mesh: ang: 16 (over z, x, core), strip: 2 (over y).
Axes of the slice: x: 2, y: 2, z: 4, core: 2. Of those that a mesh axis runs over, the one named last changes fastest.
Arguments:
- measured: float32 [16, 16, 128, 128], P('ang', 'strip'), may hold values from 0.05 to 4
- positions: int32 [16, 16], P('ang', 'strip'), may hold values from 0 to 384
- probe_field: float32 [2, 128, 128], replicated, may hold values from -6 to 6
- object_field: float32 [16, 512, 2, 128], P('ang', 'strip'), may hold values from -6 to 6
- dual_field: float32 [16, 512, 2, 128], P('ang', 'strip'), may hold values from -6 to 6
- volume: float32 [8192, 2, 128], P(('ang', 'strip')), may hold values from -6 to 6
- radon_tiles: bfloat16 [32, 16, 2, 32, 256], P(('ang', 'strip')), may hold values from -0.1875 to 0.1875
- tile_range: int32 [16, 16, 2, 1], P('ang', None, 'strip'), may hold values from 0 to 14
Outputs:
- object_next: float32 [16, 512, 2, 128], P('ang', 'strip')
- dual_next: float32 [16, 512, 2, 128], P('ang', 'strip')
- volume_next: float32 [8192, 2, 128], P(('ang', 'strip'))
The draws below stay inside these ranges and needn't reach their ends.
Inputs may be any that keep to these rules, and one draw needn't show every extreme that they name: `positions`: a frame covers 128 detector columns from its position. A pixel tile meets ray tiles tile_range to tile_range + 1 at that angle.
All inputs are finite; a program needn't handle non-finite values.
Results may differ from the reference program's by a relative error of at most 0.0027.
Values may be sent and summed in bfloat16 or wider, within the bound.
A program may use at most 64 MiB of HBM per device.

```python
import math
import jax
import jax.numpy as jnp
from jax import lax

PROBE = 128
NZ = 128
NDET = 512
RAYS = 32
TILE = 256
HITS = 2
PT_DEV = 1
NANG = 16
FR = 16
NPT = 32
NPIX = 8192
NR = 16
N_ANG = 16
N_STRIP = 2


def with_ends(array, own_key, least, top_value):
    index_at = [jax.random.randint(jax.random.fold_in(own_key, axis), (), 0, length) for axis, length in enumerate(array.shape)]
    longest = array.shape.index(max(array.shape))
    next_to = index_at[:longest] + [(index_at[longest] + 1) % array.shape[longest]] + index_at[longest + 1:]
    return array.at[tuple(index_at)].set(least).at[tuple(next_to)].set(top_value)


def steps_of(stream_key, shape, split, low, largest):
    factor_of = 1.0
    for axis_at, parts in split:
        heights = jax.random.uniform(jax.random.fold_in(jax.random.fold_in(stream_key, 6), axis_at), (parts,), jnp.float32, low / len(split), largest / len(split))
        factor_of = factor_of * jnp.repeat(jnp.exp(heights), shape[axis_at] // parts).reshape((-1,) + (1,) * (len(shape) - 1 - axis_at))
    return factor_of


def noise(key, shape, scale, most, cuts=(), kind=jnp.bfloat16):
    gain = steps_of(key, shape, cuts, -0.22, 0.18) if cuts else 1.0
    result = jax.random.normal(key, shape, jnp.float32) * scale * gain
    return jnp.minimum(jnp.maximum(result, -most), most).astype(kind)


def setup_inputs(seed: int = 0) -> dict:
    key_of = jax.random.split(jax.random.key(seed), 9)
    return {
        "measured": jnp.clip(jnp.exp(math.log(4.0) - 4.3820266 * jax.random.uniform(key_of[0], (NANG, FR, PROBE, PROBE), jnp.float32) ** steps_of(key_of[0], (NANG, FR, PROBE, PROBE), ((0, 16), (1, 2)), -0.2, 0.2)), 0.05, 4.0),
        "positions": with_ends(jax.random.randint(key_of[1], (NANG, FR), 0, NDET - PROBE + 1), jax.random.fold_in(key_of[1], 1), 0, NDET - PROBE).astype(jnp.int32),
        "probe_field": noise(key_of[2], (2, PROBE, PROBE), 1.0, 6.0, (), jnp.float32),
        "object_field": noise(key_of[3], (NANG, NDET, 2, NZ), 1.0, 6.0, ((0, 16), (1, 2)), jnp.float32),
        "dual_field": noise(key_of[4], (NANG, NDET, 2, NZ), 1.0, 6.0, ((0, 16), (1, 2)), jnp.float32),
        "volume": noise(key_of[5], (NPIX, 2, NZ), 1.0, 6.0, ((0, 32),), jnp.float32),
        "radon_tiles": noise(key_of[6], (NPT, NANG, HITS, RAYS, TILE), (HITS * NPT * TILE // NR) ** -0.5, 0.1875, ((0, 32),)),
        "tile_range": with_ends(jax.random.randint(key_of[7], (NANG, N_ANG, N_STRIP, PT_DEV), 0, NR - HITS + 1), jax.random.fold_in(key_of[7], 1), 0, NR - HITS).astype(jnp.int32),
    }


penalty = 1.0
object_step = 0.1
volume_step = 1.0
precise = lax.Precision.HIGHEST

def dft_tables(length):
    indices = jnp.arange(length, dtype=jnp.int32)
    phases = indices[:, None] * indices[None, :] % length
    angles = phases.astype(jnp.float32) * (2.0 * math.pi / length)
    scaling = 1.0 / math.sqrt(length)
    return (jnp.cos(angles) * scaling, jnp.sin(angles) * scaling)

def transform(real_part, imag_part, cosine_table, sine_table, handed):
    left_re = jnp.einsum('kc,fcr->fkr', cosine_table, real_part, precision=precise) + handed * jnp.einsum('kc,fcr->fkr', sine_table, imag_part, precision=precise)
    left_im = jnp.einsum('kc,fcr->fkr', cosine_table, imag_part, precision=precise) - handed * jnp.einsum('kc,fcr->fkr', sine_table, real_part, precision=precise)
    out_re = jnp.einsum('fkr,rl->fkl', left_re, cosine_table, precision=precise) + handed * jnp.einsum('fkr,rl->fkl', left_im, sine_table, precision=precise)
    out_im = jnp.einsum('fkr,rl->fkl', left_im, cosine_table, precision=precise) - handed * jnp.einsum('fkr,rl->fkl', left_re, sine_table, precision=precise)
    return (out_re, out_im)

def intersection_gradient(intensity, starts, field, probe_field, cosine_table, sine_table):
    window = probe_field.shape[1]

    def cutout(start):
        return lax.dynamic_slice_in_dim(field, start, window, 0)
    patches = jax.vmap(cutout)(starts)
    object_re = patches[:, :, 0, :]
    object_im = patches[:, :, 1, :]
    probe_re = probe_field[0]
    probe_im = probe_field[1]
    wave_re = probe_re * object_re - probe_im * object_im
    wave_im = probe_re * object_im + probe_im * object_re
    far_re, far_im = transform(wave_re, wave_im, cosine_table, sine_table, 1.0)
    modulus = jnp.sqrt(far_re * far_re + far_im * far_im)
    shrink = 1.0 - jnp.sqrt(intensity) / jnp.maximum(modulus, 1.0)
    back_re, back_im = transform(far_re * shrink, far_im * shrink, cosine_table, sine_table, -1.0)
    grad_re = probe_re * back_re + probe_im * back_im
    grad_im = probe_re * back_im - probe_im * back_re
    frame_grads = jnp.stack([grad_re, grad_im], axis=2)

    def deposit(index, total):
        piece = lax.dynamic_slice_in_dim(total, starts[index], window, 0)
        return lax.dynamic_update_slice_in_dim(total, piece + frame_grads[index], starts[index], 0)
    return lax.fori_loop(0, starts.shape[0], deposit, jnp.zeros(field.shape, jnp.float32))

def reference(measured, positions, probe_field, object_field, dual_field, volume, radon_tiles, tile_range):
    cosine_table, sine_table = dft_tables(PROBE)

    def ptycho_angle(inputs):
        intensity, starts, field = inputs
        return intersection_gradient(intensity, starts, field, probe_field, cosine_table, sine_table)
    intersection = lax.map(ptycho_angle, (measured, positions, object_field))
    volume_half = lax.optimization_barrier(volume.astype(jnp.bfloat16)).astype(jnp.float32).reshape(NPT, TILE, 2 * NZ)
    ranges = tile_range.reshape(NANG, NPT)
    hit_offsets = jnp.arange(HITS, dtype=jnp.int32)
    range_ids = jnp.arange(NR, dtype=jnp.int32)

    def tiles_at(angle_index):
        return lax.dynamic_index_in_dim(radon_tiles, angle_index, 1, keepdims=False).astype(jnp.float32)

    def targets_at(angle_index):
        return (ranges[angle_index][:, None] + hit_offsets[None, :]).reshape(NPT * HITS)

    def project_angle(angle_index):
        partials = jnp.einsum('phrt,ptc->phrc', tiles_at(angle_index), volume_half, precision=precise)
        selector = (range_ids[:, None] == targets_at(angle_index)[None, :]).astype(jnp.float32)
        dense_rows = jnp.dot(selector, partials.reshape(NPT * HITS, RAYS * 2 * NZ), precision=precise)
        return dense_rows.reshape(NDET, 2, NZ)
    projection = lax.map(project_angle, jnp.arange(NANG, dtype=jnp.int32))
    object_next = object_field - object_step * (intersection + dual_field + penalty * (object_field - projection))
    dual_next = dual_field + penalty * (object_next - projection)
    residual = lax.optimization_barrier((penalty * (projection - object_next) - dual_field).astype(jnp.bfloat16)).astype(jnp.float32)

    def back_angle(total, angle_index):
        selector = (targets_at(angle_index)[:, None] == range_ids[None, :]).astype(jnp.float32)
        rows = residual[angle_index].reshape(NR, RAYS * 2 * NZ)
        picked = jnp.dot(selector, rows, precision=precise).reshape(NPT, HITS, RAYS, 2 * NZ)
        return (total + jnp.einsum('phrt,phrc->ptc', tiles_at(angle_index), picked, precision=precise), None)
    gradient, unused = lax.scan(back_angle, jnp.zeros((NPT, TILE, 2 * NZ), jnp.float32), jnp.arange(NANG, dtype=jnp.int32))
    volume_next = volume - volume_step * gradient.reshape(NPIX, 2, NZ)
    return (object_next, dual_next, volume_next)
```

```python
import functools
import math

import jax
import jax.numpy as jnp
import numpy as np
from jax import lax
from jax.experimental import pallas as pl
from jax.experimental.pallas import tpu as pltpu
from jax.sharding import PartitionSpec as P

RAYS = 32
VMEM_BYTES = 67043328 - 2 * 1024 * 1024

penalty = 1.0
object_step = 0.1
volume_step = 1.0
MESH = pl.DeviceIdType.MESH


def dft_tables(length):
    indices = np.arange(length, dtype=np.int64)
    angles = (indices[:, None] * indices[None, :] % length) * (2.0 * math.pi / length)
    scaling = 1.0 / math.sqrt(length)
    parts = []
    for table in (np.cos(angles) * scaling, np.sin(angles) * scaling):
        table = table.astype(np.float32)
        high = table.astype(jnp.bfloat16)
        parts += [high, (table - high.astype(np.float32)).astype(jnp.bfloat16)]
    return np.stack(parts)


def split(value):
    high = value.astype(jnp.bfloat16)
    return high, (value - high.astype(jnp.float32)).astype(jnp.bfloat16)


def dot(left, right):
    return jnp.dot(left, right, preferred_element_type=jnp.float32)


def dot3(left, right):
    return dot(left[0], right[0]) + (dot(left[0], right[1]) + dot(left[1], right[0]))


def beside(left, right):
    return jnp.concatenate([left, right], axis=1)


def above(top, low):
    return jnp.concatenate([top, low], axis=0)


def swap_blocks(value):
    half = value.shape[1] // 2
    return above(
        beside(value[:half, :half], value[half:, :half]),
        beside(value[:half, half:], value[half:, half:]),
    )


def both_parts(ref, columns):
    return beside(ref[pl.ds(0, columns, stride=2), :], ref[pl.ds(1, columns, stride=2), :])


def put_parts(ref, value):
    columns, half = value.shape[0], value.shape[1] // 2
    ref[pl.ds(0, columns, stride=2), :] = value[:, :half]
    ref[pl.ds(1, columns, stride=2), :] = value[:, half:]


def window(start, count, rows):
    first = lax.broadcasted_iota(jnp.int32, (count, rows), 0) + start
    return one_where(first == lax.broadcasted_iota(jnp.int32, (count, rows), 1))


def one_where(mask):
    return jnp.where(mask, 1.0, 0.0).astype(jnp.bfloat16)


def one_hot(rows, starts, count, width, scale):
    lanes = lax.broadcasted_iota(jnp.int32, (1, count * width), 1)
    block = lanes // width
    target = lanes % width
    for k in range(count):
        target = target + jnp.where(block == k, starts[k] * scale, 0)
    row = lax.broadcasted_iota(jnp.int32, (rows, count * width), 0)
    return one_where(row == target)


def xor(left, right, bound):
    result, bit = 0, 1
    while bit < bound:
        result = result + ((left // bit) + (right // bit)) % 2 * bit
        bit *= 2
    return result


def kernel(
    angles, strips,
    positions, ranges, measured_hbm, probe_hbm, field_hbm, dual_hbm, volume_hbm, radon_hbm,
    tables_hbm,
    object_next, dual_next, volume_next,
    measured, probe, field, dual, volume, radon, tables,
    ray_out, ray_in, pick_out, pick_in, field_out, field_in, grad_out, grad_in,
    dense_out, dense_in, rows_half, whole_field, grads, total_grad, total_rays, turned_radon,
    picker, selector,
    load_sem, ray_send, ray_recv, pick_send, pick_recv, strip_send, strip_recv,
):
    loads = {}
    for k, (name, source, target) in enumerate((
        ("volume", volume_hbm, volume), ("radon", radon_hbm, radon), ("field", field_hbm, field),
        ("tables", tables_hbm, tables), ("probe", probe_hbm, probe),
        ("measured", measured_hbm, measured), ("dual", dual_hbm, dual),
    )):
        loads[name] = pltpu.make_async_copy(source, target, load_sem.at[k])
        loads[name].start()
    me, strip = lax.axis_index("ang"), lax.axis_index("strip")
    columns = field.shape[0] // 2
    detector = strips * columns
    frames, side = measured.shape[0], measured.shape[1]
    slices = field.shape[1]
    chunks, hit_rows = ray_out.shape[0], ray_out.shape[2]
    if angles & (angles - 1):
        ang_peers = [lax.rem(me + offset, angles) for offset in range(1, angles)]
    else:
        ang_peers = [xor(me, offset, angles) for offset in range(angles - 1, 0, -1)]
    strip_peers = [lax.rem(strip + offset, strips) for offset in range(1, strips)]

    def rows_of(owner):
        return pl.ds(pl.multiple_of(owner * columns, columns), columns)

    barrier = pltpu.get_barrier_semaphore()
    for peer in ang_peers:
        pl.semaphore_signal(barrier, inc=1, device_id=(peer, strip), device_id_type=MESH)
    for peer in strip_peers:
        pl.semaphore_signal(barrier, inc=1, device_id=(me, peer), device_id_type=MESH)

    loads["volume"].wait()
    loads["radon"].wait()
    pixels = volume.shape[0] // 2
    volume_half = both_parts(volume, pixels).astype(jnp.bfloat16)
    sums = dot(radon[...], volume_half).astype(jnp.bfloat16)
    for c in range(chunks):
        ray_out[c] = sums[:, c * slices:(c + 1) * slices].reshape(ray_out.shape[1:])
    loads["field"].wait()
    own_field = both_parts(field, columns)
    field_out[...] = own_field.astype(jnp.bfloat16)
    pl.semaphore_wait(barrier, len(ang_peers) + len(strip_peers))

    def strip_copy(source, target, stage, slot, peer):
        return pltpu.make_async_remote_copy(
            src_ref=source, dst_ref=target,
            send_sem=strip_send.at[stage, peer], recv_sem=strip_recv.at[stage, slot],
            device_id=(me, peer), device_id_type=MESH,
        )

    def ray_copy(c, slot, peer):
        return pltpu.make_async_remote_copy(
            src_ref=ray_out.at[c, peer], dst_ref=ray_in.at[c, slot],
            send_sem=ray_send.at[c, peer], recv_sem=ray_recv.at[c, slot],
            device_id=(peer, strip), device_id_type=MESH,
        )

    def pick_copy(c, slot, peer):
        return pltpu.make_async_remote_copy(
            src_ref=pick_out.at[c, peer], dst_ref=pick_in.at[c, slot],
            send_sem=pick_send.at[c, peer], recv_sem=pick_recv.at[c, slot],
            device_id=(peer, strip), device_id_type=MESH,
        )

    def grad_copy(c, slot, peer):
        return strip_copy(grad_out.at[c, peer], grad_in.at[c, slot], 1 + c, slot, peer)

    def dense_copy(c, slot, peer):
        return strip_copy(
            dense_out.at[c, peer], dense_in.at[c, slot], 1 + chunks + c, slot, peer
        )

    def residual_copy(c, owner, peer):
        part = rows_half.at[c, rows_of(owner), :]
        return strip_copy(part, part, 1 + 2 * chunks + c, owner, peer)

    started = []

    def start(copy):
        copy.start()
        started.append(copy)

    for peer in ang_peers:
        start(ray_copy(0, me, peer))
    for peer in strip_peers:
        start(strip_copy(field_out, field_in.at[strip], 0, strip, peer))
    for c in range(1, chunks):
        for peer in ang_peers:
            start(ray_copy(c, me, peer))

    for c in range(chunks):
        ray_in[c, me] = ray_out[c, me]
    selector[...] = one_hot(
        detector, [ranges[k] for k in range(angles)], angles, hit_rows, RAYS
    )
    for name in ("tables", "probe", "measured", "dual"):
        loads[name].wait()
    cos_high, cos_low, sin_high, sin_low = (tables[k] for k in range(4))
    turn = tuple(
        above(beside(c, -s), beside(s, c)) for c, s in ((cos_high, sin_high), (cos_low, sin_low))
    )
    back_turn = tuple(
        above(beside(c, s), beside(-s, c)) for c, s in ((cos_high, sin_high), (cos_low, sin_low))
    )
    probe_re, probe_im = probe[0], probe[1]
    whole_field[rows_of(strip), :] = own_field
    for peer in strip_peers:
        strip_copy(field_out, field_in.at[peer], 0, peer, peer).wait_recv()
        whole_field[rows_of(peer), :] = field_in[peer].astype(jnp.float32)
    field_high, field_low = split(whole_field[...])

    def frame_pair(pair):
        waves = []
        for j in (pair, pair + 1):
            cut = window(positions[j], side, detector)
            patch = dot(cut, field_high) + dot(cut, field_low)
            re, im = patch[:, :side], patch[:, side:]
            waves.append(beside(probe_re * re - probe_im * im, probe_re * im + probe_im * re))
        right = dot3(split(above(*waves)), turn)
        far = dot3(back_turn, split(swap_blocks(right)))
        far_re, far_im = far[:side], far[side:]
        modulus = jnp.sqrt(far_re * far_re + far_im * far_im)
        intensity = beside(measured[pair], measured[pair + 1])
        shrink = 1.0 - jnp.sqrt(intensity) / jnp.maximum(modulus, 1.0)
        left = dot3(turn, split(above(far_re * shrink, far_im * shrink)))
        back = dot3(split(swap_blocks(left)), back_turn)
        for k in range(2):
            part = back[k * side:(k + 1) * side]
            re, im = part[:, :side], part[:, side:]
            grads[(pair + k) * side:(pair + k + 1) * side, :] = beside(
                probe_re * re + probe_im * im, probe_re * im - probe_im * re
            )

    def sum_rays(c):
        for peer in ang_peers:
            ray_copy(c, peer, peer).wait_recv()
        total_rays[c] = dot(selector[...], ray_in[c].reshape(angles * hit_rows, slices))
        for k in range(strips):
            dense_out[c, k] = total_rays[c, k * columns:(k + 1) * columns].astype(jnp.bfloat16)
        for peer in strip_peers:
            start(dense_copy(c, strip, peer))

    middle = frames // 4 * 2
    for pair in range(0, middle, 2):
        frame_pair(pair)
    sum_rays(0)
    for pair in range(middle, frames, 2):
        frame_pair(pair)
    deposit = one_hot(detector, [positions[j] for j in range(frames)], frames, side, 1)
    high, low = split(grads[...])
    deposited = dot(deposit, high) + dot(deposit, low)
    for c in range(chunks):
        total_grad[c] = deposited[:, c * slices:(c + 1) * slices]
        for k in range(strips):
            grad_out[c, k] = total_grad[c, k * columns:(k + 1) * columns].astype(jnp.bfloat16)
        for peer in strip_peers:
            start(grad_copy(c, strip, peer))
    for c in range(1, chunks):
        sum_rays(c)
    for k in range(angles):
        picker[k] = window(ranges[k] * RAYS, hit_rows, detector)

    for c in range(chunks):
        intersection = total_grad[c, rows_of(strip), :]
        for peer in strip_peers:
            grad_copy(c, peer, peer).wait_recv()
            intersection = intersection + grad_in[c, peer].astype(jnp.float32)
        projection = total_rays[c, rows_of(strip), :]
        for peer in strip_peers:
            dense_copy(c, peer, peer).wait_recv()
            projection = projection + dense_in[c, peer].astype(jnp.float32)
        part = pl.ds(c, columns, stride=chunks)
        part_field, part_dual = field[part, :], dual[part, :]
        updated = part_field - object_step * (
            intersection + part_dual + penalty * (part_field - projection)
        )
        residual = penalty * (projection - updated) - part_dual
        rows_half[c, rows_of(strip), :] = residual.astype(jnp.bfloat16)
        for peer in strip_peers:
            start(residual_copy(c, strip, peer))
        object_next[part, :] = updated
        dual_next[part, :] = part_dual + penalty * (updated - projection)
    for c in range(chunks):
        for peer in strip_peers:
            residual_copy(c, peer, peer).wait_recv()
        rows = rows_half[c]
        for peer in ang_peers:
            pick_out[c, peer] = dot(picker[peer], rows).astype(jnp.bfloat16)
            start(pick_copy(c, me, peer))
        pick_in[c, me] = dot(picker[me], rows).astype(jnp.bfloat16)
    turned_radon[...] = radon[...].T
    for c in range(chunks):
        for peer in ang_peers:
            pick_copy(c, peer, peer).wait_recv()
        gradient = dot(turned_radon[...], pick_in[c].reshape(angles * hit_rows, slices))
        part = pl.ds(c, pixels, stride=chunks)
        volume_next[part, :] = volume[part, :] - volume_step * gradient
    for copy in started:
        copy.wait_send()


def finish(a, b, c, x, y, z, sem):
    copies = [
        pltpu.make_async_copy(s, t, sem.at[k]) for k, (s, t) in enumerate(((a, x), (b, y), (c, z)))
    ]
    for copy in copies:
        copy.start()
    for copy in copies:
        copy.wait()


def body(
    measured, positions, probe_field, object_field, dual_field, volume, radon_tiles, tile_range
):
    angles, strips = lax.axis_size("ang"), lax.axis_size("strip")
    frames, side = measured.shape[1], measured.shape[2]
    columns, width = object_field.shape[1], object_field.shape[2] * object_field.shape[3]
    hit_rows = radon_tiles.shape[2] * radon_tiles.shape[3]
    pixels = radon_tiles.shape[4]
    chunks, slices = object_field.shape[2], object_field.shape[3]
    vmem = pl.BlockSpec(memory_space=pltpu.VMEM)
    smem = pl.BlockSpec(memory_space=pltpu.SMEM)
    half = jnp.bfloat16
    outs = pl.pallas_call(
        functools.partial(kernel, angles, strips),
        out_shape=(
            pltpu.VMEM((2 * columns, slices), jnp.float32),
            pltpu.VMEM((2 * columns, slices), jnp.float32),
            pltpu.VMEM((2 * pixels, slices), jnp.float32),
        ),
        in_specs=[smem, smem] + [pl.BlockSpec(memory_space=pltpu.HBM)] * 7,
        out_specs=(vmem, vmem, vmem),
        scratch_shapes=[
            pltpu.VMEM((frames, side, side), jnp.float32),
            pltpu.VMEM((chunks, side, side), jnp.float32),
            pltpu.VMEM((chunks * columns, slices), jnp.float32),
            pltpu.VMEM((chunks * columns, slices), jnp.float32),
            pltpu.VMEM((chunks * pixels, slices), jnp.float32),
            pltpu.VMEM((angles * hit_rows, pixels), half),
            pltpu.VMEM((4, side, side), half),
        ] + [pltpu.VMEM((chunks, angles, hit_rows, slices), half)] * 4 + [
            pltpu.VMEM((columns, width), half),
            pltpu.VMEM((strips, columns, width), half),
        ] + [pltpu.VMEM((chunks, strips, columns, slices), half)] * 4 + [
            pltpu.VMEM((chunks, strips * columns, slices), half),
            pltpu.VMEM((strips * columns, width), jnp.float32),
            pltpu.VMEM((frames * side, width), jnp.float32),
            pltpu.VMEM((chunks, strips * columns, slices), jnp.float32),
            pltpu.VMEM((chunks, strips * columns, slices), jnp.float32),
            pltpu.VMEM((pixels, angles * hit_rows), half),
            pltpu.VMEM((angles, hit_rows, strips * columns), half),
            pltpu.VMEM((strips * columns, angles * hit_rows), half),
            pltpu.SemaphoreType.DMA((7,)),
        ] + [pltpu.SemaphoreType.DMA((chunks, angles))] * 4
        + [pltpu.SemaphoreType.DMA((1 + 3 * chunks, strips))] * 2,
        compiler_params=pltpu.CompilerParams(
            collective_id=0, has_side_effects=True, vmem_limit_bytes=VMEM_BYTES
        ),
    )(
        positions.reshape(frames),
        tile_range.reshape(angles),
        measured[0],
        probe_field,
        object_field.reshape(2 * columns, slices),
        dual_field.reshape(2 * columns, slices),
        volume.reshape(2 * pixels, slices),
        radon_tiles.reshape(angles * hit_rows, pixels),
        jnp.asarray(dft_tables(side)),
    )
    outs = pl.pallas_call(
        finish,
        out_shape=[jax.ShapeDtypeStruct(o.shape, o.dtype) for o in outs],
        in_specs=[pl.BlockSpec(memory_space=pl.ANY)] * 3,
        out_specs=[pl.BlockSpec(memory_space=pl.ANY)] * 3,
        scratch_shapes=[pltpu.SemaphoreType.DMA((3,))],
        compiler_params=pltpu.CompilerParams(vmem_limit_bytes=2 * 1024 * 1024),
    )(*outs)
    return (
        outs[0].reshape(object_field.shape),
        outs[1].reshape(dual_field.shape),
        outs[2].reshape(volume.shape),
    )


def solution(mesh):
    return jax.shard_map(
        body,
        mesh=mesh,
        in_specs=(
            P("ang", "strip", None, None),
            P("ang", "strip"),
            P(),
            P("ang", "strip", None, None),
            P("ang", "strip", None, None),
            P(("ang", "strip"), None, None),
            P(("ang", "strip"), None, None, None, None),
            P("ang", None, "strip", None),
        ),
        out_specs=(
            P("ang", "strip", None, None),
            P("ang", "strip", None, None),
            P(("ang", "strip"), None, None),
        ),
        check_vma=False,
    )
```

```python
import functools
import math

import jax
import jax.numpy as jnp
import numpy as np
from jax import lax
from jax.experimental import pallas as pl
from jax.experimental.pallas import tpu as pltpu
from jax.sharding import PartitionSpec as P

RAYS = 32
BLOCK = 128
VMEM_BYTES = 67043328 - 2 * 1024 * 1024

penalty = 1.0
object_step = 0.1
volume_step = 1.0
MESH = pl.DeviceIdType.MESH


def dft_tables(length):
    indices = np.arange(length, dtype=np.int64)
    angles = (indices[:, None] * indices[None, :] % length) * (2.0 * math.pi / length)
    scaling = 1.0 / math.sqrt(length)
    parts = []
    for table in (np.cos(angles) * scaling, np.sin(angles) * scaling):
        table = table.astype(np.float32)
        high = table.astype(jnp.bfloat16)
        parts += [high, (table - high.astype(np.float32)).astype(jnp.bfloat16)]
    return np.stack(parts)


def split(value):
    high = value.astype(jnp.bfloat16)
    return high, (value - high.astype(jnp.float32)).astype(jnp.bfloat16)


def dot(left, right):
    return jnp.dot(left, right, preferred_element_type=jnp.float32)


def dot3(left, right):
    return dot(left[0], right[0]) + (dot(left[0], right[1]) + dot(left[1], right[0]))


def beside(left, right):
    return jnp.concatenate([left, right], axis=1)


def above(top, low):
    return jnp.concatenate([top, low], axis=0)


def swap_blocks(value):
    half = value.shape[1] // 2
    return above(
        beside(value[:half, :half], value[half:, :half]),
        beside(value[:half, half:], value[half:, half:]),
    )


def both_parts(ref, columns):
    return beside(ref[pl.ds(0, columns, stride=2), :], ref[pl.ds(1, columns, stride=2), :])


def xor(left, right, bound):
    result, bit = 0, 1
    while bit < bound:
        result = result + ((left // bit) + (right // bit)) % 2 * bit
        bit *= 2
    return result


def kernel(
    angles, strips,
    positions, ranges, measured_hbm, probe_hbm, field_hbm, dual_hbm, volume_hbm, radon_hbm,
    tables_hbm,
    object_next, dual_next, volume_next,
    measured, probe, field, dual, volume, radon, tables,
    ray_out, ray_in, pick_out, pick_in, field_out, field_in, grad_out, grad_in,
    dense_out, dense_in, rows_half, whole_field, grads, own_grad, own_rays, turned_radon,
    load_sem, ray_send, ray_recv, pick_send, pick_recv, strip_send, strip_recv,
):
    loads = {}
    for k, (name, source, target) in enumerate((
        ("volume", volume_hbm, volume), ("radon", radon_hbm, radon), ("field", field_hbm, field),
        ("tables", tables_hbm, tables), ("probe", probe_hbm, probe),
        ("measured", measured_hbm, measured), ("dual", dual_hbm, dual),
    )):
        loads[name] = pltpu.make_async_copy(source, target, load_sem.at[k])
        loads[name].start()
    me, strip = lax.axis_index("ang"), lax.axis_index("strip")
    columns = field.shape[0] // 2
    detector = strips * columns
    frames, side = measured.shape[0], measured.shape[1]
    slices = field.shape[1]
    chunks, hit_rows = ray_out.shape[0], ray_out.shape[2]
    gap = detector - side
    if angles & (angles - 1):
        ang_peers = [lax.rem(me + offset, angles) for offset in range(1, angles)]
    else:
        ang_peers = [xor(me, offset, angles) for offset in range(angles - 1, 0, -1)]
    strip_peers = [lax.rem(strip + offset, strips) for offset in range(1, strips)]

    def rows_of(owner):
        return pl.ds(pl.multiple_of(owner * columns, columns), columns)

    barrier = pltpu.get_barrier_semaphore()
    for peer in ang_peers:
        pl.semaphore_signal(barrier, inc=1, device_id=(peer, strip), device_id_type=MESH)
    for peer in strip_peers:
        pl.semaphore_signal(barrier, inc=1, device_id=(me, peer), device_id_type=MESH)

    def remote(source, target, send, recv, device):
        return pltpu.make_async_remote_copy(
            src_ref=source, dst_ref=target, send_sem=send, recv_sem=recv,
            device_id=device, device_id_type=MESH,
        )

    others = pl.ds(0, angles - 1)
    slack = detector - hit_rows

    def window(slot):
        return pl.ds(pl.multiple_of(slack + slot * detector, RAYS), hit_rows)

    mates = pl.ds(0, strips - 1)

    def ray_copy(c, peer):
        return remote(
            ray_out.at[c, peer], ray_in[c].at[window(me)], ray_send.at[c], ray_recv.at[c],
            (peer, strip),
        )

    def ray_all(c):
        part = ray_in[c].at[pl.ds(0, (angles - 1) * hit_rows)]
        return remote(part, part, ray_send.at[c], ray_recv.at[c], (me, strip))

    def pick_copy(c, peer):
        return remote(
            pick_out.at[c, peer], pick_in.at[c, me], pick_send.at[c], pick_recv.at[c],
            (peer, strip),
        )

    def pick_all(c):
        return remote(
            pick_out.at[c, others], pick_in.at[c, others], pick_send.at[c], pick_recv.at[c],
            (me, strip),
        )

    def strip_copy(source, target, stage, peer):
        return remote(source, target, strip_send.at[stage], strip_recv.at[stage], (me, peer))

    def field_copy(peer):
        return strip_copy(field_out, field_in.at[strip], 0, peer)

    def grad_copy(c, peer):
        return strip_copy(grad_out.at[c, peer], grad_in.at[c, strip], 1 + c, peer)

    def dense_copy(c, peer):
        return strip_copy(dense_out.at[c, peer], dense_in.at[c, strip], 1 + chunks + c, peer)

    def residual_copy(c, peer):
        part = rows_half[c].at[rows_of(strip), :]
        return strip_copy(part, part, 1 + 2 * chunks + c, peer)

    def strip_all(ref, stage):
        return strip_copy(ref.at[mates], ref.at[mates], stage, strip)

    def residual_all(c):
        part = rows_half[c].at[pl.ds(0, (strips - 1) * columns), :]
        return strip_copy(part, part, 1 + 2 * chunks + c, strip)

    loads["field"].wait()
    for c in range(chunks):
        own = field[pl.ds(c, columns, stride=chunks), :]
        field_out[c] = own.astype(jnp.bfloat16)
        whole_field[c, rows_of(strip), :] = own
    loads["volume"].wait()
    pixels = volume.shape[0] // 2
    volume_half = both_parts(volume, pixels).astype(jnp.bfloat16)
    loads["radon"].wait()
    sums = dot(radon[...], volume_half).astype(jnp.bfloat16)
    for c in range(chunks):
        ray_out[c] = sums[:, c * slices:(c + 1) * slices].reshape(ray_out.shape[1:])
    pl.semaphore_wait(barrier, len(ang_peers) + len(strip_peers))
    for peer in strip_peers:
        field_copy(peer).start()
    for c in range(chunks):
        for peer in ang_peers:
            ray_copy(c, peer).start()

    for c in range(chunks):
        for p in range(angles + 1):
            ray_in[c][pl.ds(p * detector, slack), :] = jnp.zeros((slack, slices), jnp.bfloat16)
        ray_in[c][window(me), :] = ray_out[c, me]
        for j in range(frames + 1):
            grads[c, pl.ds(j * (gap + side), gap), :] = jnp.zeros((gap, slices), jnp.float32)
    turned_radon[...] = radon[...].T
    for name in ("tables", "probe", "measured", "dual"):
        loads[name].wait()
    cos_high, cos_low, sin_high, sin_low = (tables[k] for k in range(4))
    turn = tuple(
        above(beside(c, -s), beside(s, c)) for c, s in ((cos_high, sin_high), (cos_low, sin_low))
    )
    back_turn = tuple(
        above(beside(c, s), beside(-s, c)) for c, s in ((cos_high, sin_high), (cos_low, sin_low))
    )
    probe_re, probe_im = probe[0], probe[1]
    strip_all(field_in, 0).wait_recv()
    for peer in strip_peers:
        for c in range(chunks):
            whole_field[c, rows_of(peer), :] = field_in[peer, c].astype(jnp.float32)

    def frame_pair(pair):
        waves = []
        for j in (pair, pair + 1):
            re = whole_field[0, pl.ds(positions[j], side), :]
            im = whole_field[1, pl.ds(positions[j], side), :]
            waves.append(beside(probe_re * re - probe_im * im, probe_re * im + probe_im * re))
        right = dot3(split(above(*waves)), turn)
        far = dot3(back_turn, split(swap_blocks(right)))
        far_re, far_im = far[:side], far[side:]
        modulus = jnp.sqrt(far_re * far_re + far_im * far_im)
        intensity = beside(measured[pair], measured[pair + 1])
        shrink = 1.0 - jnp.sqrt(intensity) / jnp.maximum(modulus, 1.0)
        left = dot3(turn, split(above(far_re * shrink, far_im * shrink)))
        back = dot3(split(swap_blocks(left)), back_turn)
        for k in range(2):
            part = back[k * side:(k + 1) * side]
            re, im = part[:, :side], part[:, side:]
            rows = pl.ds(gap + (pair + k) * (gap + side), side)
            grads[0, rows, :] = probe_re * re + probe_im * im
            grads[1, rows, :] = probe_re * im - probe_im * re

    def deposit(c, first, rows):
        total = None
        for j in range(frames):
            start = gap + j * (gap + side) + first - positions[j]
            piece = grads[c, pl.ds(start, rows), :]
            total = piece if total is None else total + piece
        return total

    def sum_tile(c, tile):
        total = None
        for p in range(angles):
            start = ((slack + p * detector) // RAYS + tile - ranges[p]) * RAYS
            piece = ray_in[c][pl.ds(start, RAYS), :].astype(jnp.float32)
            total = piece if total is None else total + piece
        return total

    block = min(BLOCK, columns)

    def send_grads(c):
        for peer in strip_peers:
            for k in range(columns // block):
                grad_out[c, peer, pl.ds(k * block, block), :] = deposit(
                    c, peer * columns + k * block, block
                ).astype(jnp.bfloat16)
            grad_copy(c, peer).start()
        for k in range(columns // block):
            own_grad[c, pl.ds(k * block, block), :] = deposit(
                c, strip * columns + k * block, block
            )

    def send_rays(c):
        ray_all(c).wait_recv()
        tiles = columns // RAYS
        for peer in strip_peers:
            for k in range(tiles):
                dense_out[c, peer, pl.ds(k * RAYS, RAYS), :] = sum_tile(
                    c, peer * tiles + k
                ).astype(jnp.bfloat16)
            dense_copy(c, peer).start()
        for k in range(tiles):
            own_rays[c, pl.ds(k * RAYS, RAYS), :] = sum_tile(c, strip * tiles + k)

    def update(c):
        strip_all(grad_in.at[c], 1 + c).wait_recv()
        strip_all(dense_in.at[c], 1 + chunks + c).wait_recv()
        for k in range(columns // block):
            here = pl.ds(k * block, block)
            intersection, projection = own_grad[c, here, :], own_rays[c, here, :]
            for peer in strip_peers:
                intersection = intersection + grad_in[c, peer, here, :].astype(jnp.float32)
                projection = projection + dense_in[c, peer, here, :].astype(jnp.float32)
            part = pl.ds(c + k * block * chunks, block, stride=chunks)
            part_field, part_dual = field[part, :], dual[part, :]
            updated = part_field - object_step * (
                intersection + part_dual + penalty * (part_field - projection)
            )
            residual = penalty * (projection - updated) - part_dual
            rows_half[c][pl.ds(pl.multiple_of(strip * columns + k * block, block), block), :] = (
                residual.astype(jnp.bfloat16)
            )
            object_next[part, :] = updated
            dual_next[part, :] = part_dual + penalty * (updated - projection)
        for peer in strip_peers:
            residual_copy(c, peer).start()

    def send_picks(c):
        residual_all(c).wait_recv()
        for peer in ang_peers:
            pick_out[c, peer] = rows_half[c][pl.ds(ranges[peer] * RAYS, hit_rows), :]
            pick_copy(c, peer).start()
        pick_in[c, me] = rows_half[c][pl.ds(ranges[me] * RAYS, hit_rows), :]

    for pair in range(0, frames, 2):
        frame_pair(pair)
    send_grads(0)
    send_rays(0)
    for c in range(1, chunks):
        send_grads(c)
    for c in range(chunks):
        update(c)
        send_picks(c)
        if c + 1 < chunks:
            send_rays(c + 1)
    for c in range(chunks):
        pick_all(c).wait_recv()
        gradient = dot(turned_radon[...], pick_in[c].reshape(angles * hit_rows, slices))
        part = pl.ds(c, pixels, stride=chunks)
        volume_next[part, :] = volume[part, :] - volume_step * gradient
    for peer in strip_peers:
        field_copy(peer).wait_send()
    for c in range(chunks):
        ray_all(c).wait_send()
        pick_all(c).wait_send()
        strip_all(grad_out.at[c], 1 + c).wait_send()
        strip_all(dense_out.at[c], 1 + chunks + c).wait_send()
        for peer in strip_peers:
            residual_copy(c, peer).wait_send()


def finish(first, second, third, first_out, second_out, third_out, sem):
    copies = [
        pltpu.make_async_copy(source, target, sem.at[k])
        for k, (source, target) in enumerate(
            ((first, first_out), (second, second_out), (third, third_out))
        )
    ]
    for copy in copies:
        copy.start()
    for copy in copies:
        copy.wait()


def body(
    measured, positions, probe_field, object_field, dual_field, volume, radon_tiles, tile_range
):
    angles, strips = lax.axis_size("ang"), lax.axis_size("strip")
    frames, side = measured.shape[1], measured.shape[2]
    columns = object_field.shape[1]
    hit_rows = radon_tiles.shape[2] * radon_tiles.shape[3]
    pixels = radon_tiles.shape[4]
    chunks, slices = object_field.shape[2], object_field.shape[3]
    detector = strips * columns
    pad_rows = detector - side + frames * detector
    half = jnp.bfloat16
    outs = pl.pallas_call(
        functools.partial(kernel, angles, strips),
        out_shape=(
            pltpu.VMEM((chunks * columns, slices), jnp.float32),
            pltpu.VMEM((chunks * columns, slices), jnp.float32),
            pltpu.VMEM((chunks * pixels, slices), jnp.float32),
        ),
        in_specs=[pl.BlockSpec(memory_space=pltpu.SMEM)] * 2
        + [pl.BlockSpec(memory_space=pltpu.HBM)] * 7,
        out_specs=(pl.BlockSpec(memory_space=pltpu.VMEM),) * 3,
        scratch_shapes=[
            pltpu.VMEM((frames, side, side), jnp.float32),
            pltpu.VMEM((chunks, side, side), jnp.float32),
            pltpu.VMEM((chunks * columns, slices), jnp.float32),
            pltpu.VMEM((chunks * columns, slices), jnp.float32),
            pltpu.VMEM((chunks * pixels, slices), jnp.float32),
            pltpu.VMEM((angles * hit_rows, pixels), half),
            pltpu.VMEM((4, side, side), half),
            pltpu.VMEM((chunks, angles, hit_rows, slices), half),
            [pltpu.VMEM(((angles + 1) * detector - hit_rows, slices), half)] * chunks,
            pltpu.VMEM((chunks, angles, hit_rows, slices), half),
            pltpu.VMEM((chunks, angles, hit_rows, slices), half),
            pltpu.VMEM((chunks, columns, slices), half),
            pltpu.VMEM((strips, chunks, columns, slices), half),
        ] + [pltpu.VMEM((chunks, strips, columns, slices), half)] * 4 + [
            [pltpu.VMEM((detector, slices), half)] * chunks,
            pltpu.VMEM((chunks, detector, slices), jnp.float32),
            pltpu.VMEM((chunks, pad_rows, slices), jnp.float32),
            pltpu.VMEM((chunks, columns, slices), jnp.float32),
            pltpu.VMEM((chunks, columns, slices), jnp.float32),
            pltpu.VMEM((pixels, angles * hit_rows), half),
            pltpu.SemaphoreType.DMA((7,)),
        ] + [pltpu.SemaphoreType.DMA((chunks,))] * 4
        + [pltpu.SemaphoreType.DMA((1 + 3 * chunks,))] * 2,
        compiler_params=pltpu.CompilerParams(
            collective_id=0, has_side_effects=True, vmem_limit_bytes=VMEM_BYTES
        ),
    )(
        positions.reshape(frames),
        tile_range.reshape(angles),
        measured[0],
        probe_field,
        object_field.reshape(chunks * columns, slices),
        dual_field.reshape(chunks * columns, slices),
        volume.reshape(chunks * pixels, slices),
        radon_tiles.reshape(angles * hit_rows, pixels),
        jnp.asarray(dft_tables(side)),
    )
    outs = pl.pallas_call(
        finish,
        out_shape=[jax.ShapeDtypeStruct(o.shape, o.dtype) for o in outs],
        in_specs=[pl.BlockSpec(memory_space=pl.ANY)] * 3,
        out_specs=[pl.BlockSpec(memory_space=pl.ANY)] * 3,
        scratch_shapes=[pltpu.SemaphoreType.DMA((3,))],
        compiler_params=pltpu.CompilerParams(vmem_limit_bytes=2 * 1024 * 1024),
    )(*outs)
    return (
        outs[0].reshape(object_field.shape),
        outs[1].reshape(dual_field.shape),
        outs[2].reshape(volume.shape),
    )


def solution(mesh):
    return jax.shard_map(
        body,
        mesh=mesh,
        in_specs=(
            P("ang", "strip", None, None),
            P("ang", "strip"),
            P(),
            P("ang", "strip", None, None),
            P("ang", "strip", None, None),
            P(("ang", "strip"), None, None),
            P(("ang", "strip"), None, None, None, None),
            P("ang", None, "strip", None),
        ),
        out_specs=(
            P("ang", "strip", None, None),
            P("ang", "strip", None, None),
            P(("ang", "strip"), None, None),
        ),
        check_vma=False,
    )
```

```python
import functools
import math

import jax
import jax.numpy as jnp
import numpy as np
from jax import lax
from jax.experimental import pallas as pl
from jax.experimental.pallas import tpu as pltpu
from jax.sharding import PartitionSpec as P

RAYS = 32
VMEM_BYTES = 67043328 - 2 * 1024 * 1024

penalty = 1.0
object_step = 0.1
volume_step = 1.0
MESH = pl.DeviceIdType.MESH


def dft_tables(length):
    indices = np.arange(length, dtype=np.int64)
    angles = (indices[:, None] * indices[None, :] % length) * (2.0 * math.pi / length)
    scaling = 1.0 / math.sqrt(length)
    parts = []
    for table in (np.cos(angles) * scaling, np.sin(angles) * scaling):
        table = table.astype(np.float32)
        high = table.astype(jnp.bfloat16)
        parts += [high, (table - high.astype(np.float32)).astype(jnp.bfloat16)]
    return np.stack(parts)


def split(value):
    high = value.astype(jnp.bfloat16)
    return high, (value - high.astype(jnp.float32)).astype(jnp.bfloat16)


def dot(left, right):
    return jnp.dot(left, right, preferred_element_type=jnp.float32)


def dot3(left, right):
    return dot(left[0], right[0]) + (dot(left[0], right[1]) + dot(left[1], right[0]))


def beside(left, right):
    return jnp.concatenate([left, right], axis=1)


def above(top, low):
    return jnp.concatenate([top, low], axis=0)


def swap_blocks(value):
    half = value.shape[1] // 2
    return above(
        beside(value[:half, :half], value[half:, :half]),
        beside(value[:half, half:], value[half:, half:]),
    )


def both_parts(ref, columns):
    return beside(ref[pl.ds(0, columns, stride=2), :], ref[pl.ds(1, columns, stride=2), :])


def xor(left, right, bound):
    result, bit = 0, 1
    while bit < bound:
        result = result + ((left // bit) + (right // bit)) % 2 * bit
        bit *= 2
    return result


def kernel(
    angles, strips,
    positions_hbm, ranges_hbm, measured_hbm, probe_hbm, field_hbm, dual_hbm, volume_hbm, radon_hbm,
    tables_hbm,
    object_next, dual_next, volume_next,
    positions, ranges, measured, probe, field, dual, volume, radon, tables,
    ray_out, ray_in, pick_out, pick_in, field_out, field_in, grad_out, grad_in,
    dense_out, dense_in, mixed_out, mixed_in, rows_half, whole_field, grads,
    own_grad, own_rays, own_mixed, turned_radon,
    load_sem, ray_send, ray_recv, pick_send, pick_recv, strip_send, strip_recv,
):
    loads = {}
    for k, (name, source, target) in enumerate((
        ("field", field_hbm, field), ("volume", volume_hbm, volume), ("radon", radon_hbm, radon),
        ("positions", positions_hbm, positions), ("ranges", ranges_hbm, ranges),
        ("tables", tables_hbm, tables), ("probe", probe_hbm, probe),
        ("measured", measured_hbm, measured), ("dual", dual_hbm, dual),
    )):
        loads[name] = pltpu.make_async_copy(source, target, load_sem.at[k])
        loads[name].start()
    me, strip = lax.axis_index("ang"), lax.axis_index("strip")
    columns = field.shape[0] // 2
    detector = strips * columns
    frames, side = measured.shape[0], measured.shape[1]
    slices = field.shape[1]
    chunks, hit_rows = ray_out.shape[0], ray_out.shape[2]
    gap = detector - side
    if angles & (angles - 1):
        ang_peers = [lax.rem(me + offset, angles) for offset in range(1, angles)]
    else:
        ang_peers = [xor(me, offset, angles) for offset in range(angles - 1, 0, -1)]
    strip_peers = [lax.rem(strip + offset, strips) for offset in range(1, strips)]

    def rows_of(owner):
        return pl.ds(pl.multiple_of(owner * columns, columns), columns)

    barrier = pltpu.get_barrier_semaphore()
    for peer in ang_peers:
        pl.semaphore_signal(barrier, inc=1, device_id=(peer, strip), device_id_type=MESH)
    for peer in strip_peers:
        pl.semaphore_signal(barrier, inc=1, device_id=(me, peer), device_id_type=MESH)

    def remote(source, target, send, recv, device):
        return pltpu.make_async_remote_copy(
            src_ref=source, dst_ref=target, send_sem=send, recv_sem=recv,
            device_id=device, device_id_type=MESH,
        )

    others = pl.ds(0, angles - 1)
    slack = detector - hit_rows

    def window(slot):
        return pl.ds(pl.multiple_of(slack + slot * detector, RAYS), hit_rows)

    mates = pl.ds(0, strips - 1)

    def ray_copy(c, peer):
        return remote(
            ray_out.at[c, peer], ray_in[c].at[window(me)], ray_send.at[c], ray_recv.at[c],
            (peer, strip),
        )

    def ray_all(c):
        part = ray_in[c].at[pl.ds(0, (angles - 1) * hit_rows)]
        return remote(part, part, ray_send.at[c], ray_recv.at[c], (me, strip))

    def pick_copy(c, peer):
        return remote(
            pick_out.at[c, peer], pick_in.at[c, me], pick_send.at[c], pick_recv.at[c],
            (peer, strip),
        )

    def pick_all(c):
        return remote(
            pick_out.at[c, others], pick_in.at[c, others], pick_send.at[c], pick_recv.at[c],
            (me, strip),
        )

    def strip_copy(source, target, stage, peer):
        return remote(source, target, strip_send.at[stage], strip_recv.at[stage], (me, peer))

    def field_copy(peer):
        return strip_copy(field_out, field_in.at[strip], 0, peer)

    def grad_copy(c, peer):
        return strip_copy(grad_out.at[c, peer], grad_in.at[c, strip], 1 + c, peer)

    def dense_copy(c, peer):
        return strip_copy(dense_out.at[c, peer], dense_in.at[c, strip], 1 + chunks + c, peer)

    def residual_copy(c, peer):
        part = rows_half[c].at[rows_of(strip), :]
        return strip_copy(part, part, 1 + 2 * chunks + c, peer)

    def mixed_copy(c, peer):
        return strip_copy(mixed_out.at[c, peer], mixed_in.at[c, strip], 1 + 3 * chunks + c, peer)

    def strip_all(ref, stage):
        return strip_copy(ref.at[mates], ref.at[mates], stage, strip)

    def residual_all(c):
        part = rows_half[c].at[pl.ds(0, (strips - 1) * columns), :]
        return strip_copy(part, part, 1 + 2 * chunks + c, strip)

    loads["field"].wait()
    for c in range(chunks):
        own = field[pl.ds(c, columns, stride=chunks), :]
        field_out[c] = own.astype(jnp.bfloat16)
        whole_field[c, rows_of(strip), :] = own
    pl.semaphore_wait(barrier, len(ang_peers) + len(strip_peers))
    for peer in strip_peers:
        field_copy(peer).start()
    loads["volume"].wait()
    pixels = volume.shape[0] // 2
    volume_half = both_parts(volume, pixels).astype(jnp.bfloat16)
    loads["radon"].wait()
    sums = dot(radon[...], volume_half).astype(jnp.bfloat16)
    for c in range(chunks):
        ray_out[c] = sums[:, c * slices:(c + 1) * slices].reshape(ray_out.shape[1:])

    def start_rays(c):
        for peer in ang_peers:
            ray_copy(c, peer).start()

    start_rays(0)
    for c in range(chunks):
        for p in range(angles + 1):
            ray_in[c][pl.ds(p * detector, slack), :] = jnp.zeros((slack, slices), jnp.bfloat16)
        ray_in[c][window(me), :] = ray_out[c, me]
        for j in range(frames + 1):
            grads[c, pl.ds(j * (gap + side), gap), :] = jnp.zeros((gap, slices), jnp.float32)
    turned_radon[...] = radon[...].T
    for name in ("positions", "ranges", "tables", "probe", "measured", "dual"):
        loads[name].wait()
    cos_high, cos_low, sin_high, sin_low = (tables[k] for k in range(4))
    turn = tuple(
        above(beside(c, -s), beside(s, c)) for c, s in ((cos_high, sin_high), (cos_low, sin_low))
    )
    back_turn = tuple(
        above(beside(c, s), beside(-s, c)) for c, s in ((cos_high, sin_high), (cos_low, sin_low))
    )
    probe_re, probe_im = probe[0], probe[1]
    strip_all(field_in, 0).wait_recv()
    for peer in strip_peers:
        for c in range(chunks):
            whole_field[c, rows_of(peer), :] = field_in[peer, c].astype(jnp.float32)

    def frame_pair(pair):
        waves = []
        for j in (pair, pair + 1):
            re = whole_field[0, pl.ds(positions[j], side), :]
            im = whole_field[1, pl.ds(positions[j], side), :]
            waves.append(beside(probe_re * re - probe_im * im, probe_re * im + probe_im * re))
        right = dot3(split(above(*waves)), turn)
        far = dot3(back_turn, split(swap_blocks(right)))
        far_re, far_im = far[:side], far[side:]
        modulus = jnp.sqrt(far_re * far_re + far_im * far_im)
        intensity = beside(measured[pair], measured[pair + 1])
        shrink = 1.0 - jnp.sqrt(intensity) / jnp.maximum(modulus, 1.0)
        left = dot3(turn, split(above(far_re * shrink, far_im * shrink)))
        back = dot3(split(swap_blocks(left)), back_turn)
        for k in range(2):
            part = back[k * side:(k + 1) * side]
            re, im = part[:, :side], part[:, side:]
            rows = pl.ds(gap + (pair + k) * (gap + side), side)
            grads[0, rows, :] = probe_re * re + probe_im * im
            grads[1, rows, :] = probe_re * im - probe_im * re

    def deposit(c, first, rows):
        total = None
        for j in range(frames):
            start = gap + j * (gap + side) + first - positions[j]
            piece = grads[c, pl.ds(start, rows), :]
            total = piece if total is None else total + piece
        return total

    def sum_tile(c, tile):
        total = None
        for p in range(angles):
            start = ((slack + p * detector) // RAYS + tile - ranges[p]) * RAYS
            piece = ray_in[c][pl.ds(start, RAYS), :].astype(jnp.float32)
            total = piece if total is None else total + piece
        return total

    tiles = columns // RAYS
    ray_weight = penalty - penalty * penalty * object_step
    grad_weight = penalty * object_step
    dual_weight = 1.0 - penalty * object_step

    def tile_rows(k):
        return pl.ds(k * RAYS, RAYS)

    def send_mixed(c):
        ray_all(c).wait_recv()
        for peer in strip_peers:
            for k in range(tiles):
                rays = sum_tile(c, peer * tiles + k)
                grad = deposit(c, peer * columns + k * RAYS, RAYS)
                mixed_out[c, peer, tile_rows(k), :] = (
                    ray_weight * rays + grad_weight * grad
                ).astype(jnp.bfloat16)
                dense_out[c, peer, tile_rows(k), :] = rays.astype(jnp.bfloat16)
                grad_out[c, peer, tile_rows(k), :] = grad.astype(jnp.bfloat16)
            mixed_copy(c, peer).start()
        for k in range(tiles):
            rays = sum_tile(c, strip * tiles + k)
            grad = deposit(c, strip * columns + k * RAYS, RAYS)
            part = pl.ds(c + k * RAYS * chunks, RAYS, stride=chunks)
            own_rays[c, tile_rows(k), :] = rays
            own_grad[c, tile_rows(k), :] = grad
            own_mixed[c, tile_rows(k), :] = (
                ray_weight * rays + grad_weight * grad
                - (dual_weight * dual[part, :] + ray_weight * field[part, :])
            )

    def send_residual(c):
        strip_all(mixed_in.at[c], 1 + 3 * chunks + c).wait_recv()
        for k in range(tiles):
            residual = own_mixed[c, tile_rows(k), :]
            for peer in strip_peers:
                residual = residual + mixed_in[c, peer, tile_rows(k), :].astype(jnp.float32)
            rows_half[c][pl.ds(pl.multiple_of(strip * columns + k * RAYS, RAYS), RAYS), :] = (
                residual.astype(jnp.bfloat16)
            )
        for peer in strip_peers:
            residual_copy(c, peer).start()

    def send_parts(c):
        for peer in strip_peers:
            grad_copy(c, peer).start()
            dense_copy(c, peer).start()

    def update(c):
        strip_all(grad_in.at[c], 1 + c).wait_recv()
        strip_all(dense_in.at[c], 1 + chunks + c).wait_recv()
        for k in range(tiles):
            here = tile_rows(k)
            intersection, projection = own_grad[c, here, :], own_rays[c, here, :]
            for peer in strip_peers:
                intersection = intersection + grad_in[c, peer, here, :].astype(jnp.float32)
                projection = projection + dense_in[c, peer, here, :].astype(jnp.float32)
            part = pl.ds(c + k * RAYS * chunks, RAYS, stride=chunks)
            part_field, part_dual = field[part, :], dual[part, :]
            updated = part_field - object_step * (
                intersection + part_dual + penalty * (part_field - projection)
            )
            object_next[part, :] = updated
            dual_next[part, :] = part_dual + penalty * (updated - projection)

    def send_picks(c):
        residual_all(c).wait_recv()
        for peer in ang_peers:
            pick_out[c, peer] = rows_half[c][pl.ds(ranges[peer] * RAYS, hit_rows), :]
            pick_copy(c, peer).start()
        pick_in[c, me] = rows_half[c][pl.ds(ranges[me] * RAYS, hit_rows), :]

    for pair in range(0, frames, 2):
        frame_pair(pair)
        if pair == 0:
            for c in range(1, chunks):
                start_rays(c)
    send_mixed(0)
    for c in range(chunks):
        send_residual(c)
        if c + 1 < chunks:
            send_mixed(c + 1)
        send_picks(c)
    for c in range(chunks):
        send_parts(c)
    for c in range(chunks):
        update(c)
    for c in range(chunks):
        pick_all(c).wait_recv()
        gradient = dot(turned_radon[...], pick_in[c].reshape(angles * hit_rows, slices))
        part = pl.ds(c, pixels, stride=chunks)
        volume_next[part, :] = volume[part, :] - volume_step * gradient
    for peer in strip_peers:
        field_copy(peer).wait_send()
    for c in range(chunks):
        ray_all(c).wait_send()
        pick_all(c).wait_send()
        strip_all(grad_out.at[c], 1 + c).wait_send()
        strip_all(dense_out.at[c], 1 + chunks + c).wait_send()
        strip_all(mixed_out.at[c], 1 + 3 * chunks + c).wait_send()
        for peer in strip_peers:
            residual_copy(c, peer).wait_send()


def finish(first, second, third, first_out, second_out, third_out, sem):
    copies = [
        pltpu.make_async_copy(source, target, sem.at[k])
        for k, (source, target) in enumerate(
            ((first, first_out), (second, second_out), (third, third_out))
        )
    ]
    for copy in copies:
        copy.start()
    for copy in copies:
        copy.wait()


def body(
    measured, positions, probe_field, object_field, dual_field, volume, radon_tiles, tile_range
):
    angles, strips = lax.axis_size("ang"), lax.axis_size("strip")
    frames, side = measured.shape[1], measured.shape[2]
    columns = object_field.shape[1]
    hit_rows = radon_tiles.shape[2] * radon_tiles.shape[3]
    pixels = radon_tiles.shape[4]
    chunks, slices = object_field.shape[2], object_field.shape[3]
    detector = strips * columns
    pad_rows = detector - side + frames * detector
    half = jnp.bfloat16
    outs = pl.pallas_call(
        functools.partial(kernel, angles, strips),
        out_shape=(
            pltpu.VMEM((chunks * columns, slices), jnp.float32),
            pltpu.VMEM((chunks * columns, slices), jnp.float32),
            pltpu.VMEM((chunks * pixels, slices), jnp.float32),
        ),
        in_specs=[pl.BlockSpec(memory_space=pltpu.HBM)] * 9,
        out_specs=(pl.BlockSpec(memory_space=pltpu.VMEM),) * 3,
        scratch_shapes=[
            pltpu.SMEM((frames,), jnp.int32),
            pltpu.SMEM((angles,), jnp.int32),
            pltpu.VMEM((frames, side, side), jnp.float32),
            pltpu.VMEM((chunks, side, side), jnp.float32),
            pltpu.VMEM((chunks * columns, slices), jnp.float32),
            pltpu.VMEM((chunks * columns, slices), jnp.float32),
            pltpu.VMEM((chunks * pixels, slices), jnp.float32),
            pltpu.VMEM((angles * hit_rows, pixels), half),
            pltpu.VMEM((4, side, side), half),
            pltpu.VMEM((chunks, angles, hit_rows, slices), half),
            [pltpu.VMEM(((angles + 1) * detector - hit_rows, slices), half)] * chunks,
            pltpu.VMEM((chunks, angles, hit_rows, slices), half),
            pltpu.VMEM((chunks, angles, hit_rows, slices), half),
            pltpu.VMEM((chunks, columns, slices), half),
            pltpu.VMEM((strips, chunks, columns, slices), half),
        ] + [pltpu.VMEM((chunks, strips, columns, slices), half)] * 6 + [
            [pltpu.VMEM((detector, slices), half)] * chunks,
            pltpu.VMEM((chunks, detector, slices), jnp.float32),
            pltpu.VMEM((chunks, pad_rows, slices), jnp.float32),
            pltpu.VMEM((chunks, columns, slices), jnp.float32),
            pltpu.VMEM((chunks, columns, slices), jnp.float32),
            pltpu.VMEM((chunks, columns, slices), jnp.float32),
            pltpu.VMEM((pixels, angles * hit_rows), half),
            pltpu.SemaphoreType.DMA((9,)),
        ] + [pltpu.SemaphoreType.DMA((chunks,))] * 4
        + [pltpu.SemaphoreType.DMA((1 + 4 * chunks,))] * 2,
        compiler_params=pltpu.CompilerParams(
            collective_id=0, has_side_effects=True, vmem_limit_bytes=VMEM_BYTES
        ),
    )(
        positions.reshape(frames),
        tile_range.reshape(angles),
        measured[0],
        probe_field,
        object_field.reshape(chunks * columns, slices),
        dual_field.reshape(chunks * columns, slices),
        volume.reshape(chunks * pixels, slices),
        radon_tiles.reshape(angles * hit_rows, pixels),
        jnp.asarray(dft_tables(side)),
    )
    outs = pl.pallas_call(
        finish,
        out_shape=[jax.ShapeDtypeStruct(o.shape, o.dtype) for o in outs],
        in_specs=[pl.BlockSpec(memory_space=pl.ANY)] * 3,
        out_specs=[pl.BlockSpec(memory_space=pl.ANY)] * 3,
        scratch_shapes=[pltpu.SemaphoreType.DMA((3,))],
        compiler_params=pltpu.CompilerParams(vmem_limit_bytes=2 * 1024 * 1024),
    )(*outs)
    return (
        outs[0].reshape(object_field.shape),
        outs[1].reshape(dual_field.shape),
        outs[2].reshape(volume.shape),
    )


def solution(mesh):
    return jax.shard_map(
        body,
        mesh=mesh,
        in_specs=(
            P("ang", "strip", None, None),
            P("ang", "strip"),
            P(),
            P("ang", "strip", None, None),
            P("ang", "strip", None, None),
            P(("ang", "strip"), None, None),
            P(("ang", "strip"), None, None, None, None),
            P("ang", None, "strip", None),
        ),
        out_specs=(
            P("ang", "strip", None, None),
            P("ang", "strip", None, None),
            P(("ang", "strip"), None, None),
        ),
        check_vma=False,
    )
```

```python
import functools
import math

import jax
import jax.numpy as jnp
import numpy as np
from jax import lax
from jax.experimental import pallas as pl
from jax.experimental.pallas import tpu as pltpu
from jax.sharding import PartitionSpec as P

RAYS = 32
VMEM_BYTES = 67043328 - 2 * 1024 * 1024

penalty = 1.0
object_step = 0.1
volume_step = 1.0
MESH = pl.DeviceIdType.MESH


def dft_tables(length):
    indices = np.arange(length, dtype=np.int64)
    angles = (indices[:, None] * indices[None, :] % length) * (2.0 * math.pi / length)
    scaling = 1.0 / math.sqrt(length)
    parts = []
    for table in (np.cos(angles) * scaling, np.sin(angles) * scaling):
        table = table.astype(np.float32)
        high = table.astype(jnp.bfloat16)
        parts += [high, (table - high.astype(np.float32)).astype(jnp.bfloat16)]
    return np.stack(parts)


def split(value):
    high = value.astype(jnp.bfloat16)
    return high, (value - high.astype(jnp.float32)).astype(jnp.bfloat16)


def dot(left, right):
    return jnp.dot(left, right, preferred_element_type=jnp.float32)


def dot3(left, right):
    return dot(
        jnp.concatenate([left[0], left[0], left[1]], axis=1),
        jnp.concatenate([right[0], right[1], right[0]], axis=0),
    )


def beside(left, right):
    return jnp.concatenate([left, right], axis=1)


def above(top, low):
    return jnp.concatenate([top, low], axis=0)


def swap_blocks(value):
    half = value.shape[1] // 2
    return above(
        beside(value[:half, :half], value[half:, :half]),
        beside(value[:half, half:], value[half:, half:]),
    )


def both_parts(ref, columns):
    return beside(ref[pl.ds(0, columns, stride=2), :], ref[pl.ds(1, columns, stride=2), :])


def xor(left, right, bound):
    result, bit = 0, 1
    while bit < bound:
        result = result + ((left // bit) + (right // bit)) % 2 * bit
        bit *= 2
    return result


def kernel(
    angles, strips,
    positions_hbm, ranges_hbm, measured_hbm, probe_hbm, field_hbm, dual_hbm, volume_hbm, radon_hbm,
    tables_hbm,
    object_next, dual_next, volume_next,
    positions, ranges, measured, probe, field, dual, volume, radon, tables,
    ray_out, ray_in, pick_out, pick_in, field_out, field_in, grad_out, grad_in,
    mixed_out, mixed_in, wide, rows_half, whole_field, grads,
    own_grad, own_rays, own_mixed, turned_radon,
    load_sem, ray_send, ray_recv, pick_send, pick_recv, strip_send, strip_recv,
):
    loads = {}
    for k, (name, source, target) in enumerate((
        ("field", field_hbm, field), ("volume", volume_hbm, volume), ("radon", radon_hbm, radon),
        ("positions", positions_hbm, positions), ("ranges", ranges_hbm, ranges),
        ("tables", tables_hbm, tables), ("probe", probe_hbm, probe),
        ("measured", measured_hbm, measured), ("dual", dual_hbm, dual),
    )):
        loads[name] = pltpu.make_async_copy(source, target, load_sem.at[k])
        loads[name].start()
    me, strip = lax.axis_index("ang"), lax.axis_index("strip")
    columns = field.shape[0] // 2
    detector = strips * columns
    frames, side = measured.shape[0], measured.shape[1]
    slices = field.shape[1]
    chunks, hit_rows = ray_out.shape[0], ray_out.shape[2]
    gap = detector - side
    if angles & (angles - 1):
        ang_peers = [lax.rem(me + offset, angles) for offset in range(1, angles)]
    else:
        ang_peers = [xor(me, offset, angles) for offset in range(angles - 1, 0, -1)]
    strip_peers = [lax.rem(strip + offset, strips) for offset in range(1, strips)]

    def rows_of(owner):
        return pl.ds(pl.multiple_of(owner * columns, columns), columns)

    barrier = pltpu.get_barrier_semaphore()
    for peer in ang_peers:
        pl.semaphore_signal(barrier, inc=1, device_id=(peer, strip), device_id_type=MESH)
    for peer in strip_peers:
        pl.semaphore_signal(barrier, inc=1, device_id=(me, peer), device_id_type=MESH)

    def remote(source, target, send, recv, device):
        return pltpu.make_async_remote_copy(
            src_ref=source, dst_ref=target, send_sem=send, recv_sem=recv,
            device_id=device, device_id_type=MESH,
        )

    others = pl.ds(0, angles - 1)
    slack = detector - hit_rows

    def window(slot):
        return pl.ds(pl.multiple_of(slack + slot * detector, RAYS), hit_rows)

    mates = pl.ds(0, strips - 1)

    def ray_copy(c, peer):
        return remote(
            ray_out.at[c, peer], ray_in[c].at[window(me)], ray_send.at[c], ray_recv.at[c],
            (peer, strip),
        )

    def ray_all(c):
        part = ray_in[c].at[pl.ds(0, (angles - 1) * hit_rows)]
        return remote(part, part, ray_send.at[c], ray_recv.at[c], (me, strip))

    def pick_copy(c, peer):
        return remote(
            pick_out.at[c, peer], pick_in.at[c, me], pick_send.at[c], pick_recv.at[c],
            (peer, strip),
        )

    def pick_all(c):
        return remote(
            pick_out.at[c, others], pick_in.at[c, others], pick_send.at[c], pick_recv.at[c],
            (me, strip),
        )

    def strip_copy(source, target, stage, peer):
        return remote(source, target, strip_send.at[stage], strip_recv.at[stage], (me, peer))

    def field_copy(peer):
        return strip_copy(field_out, field_in.at[strip], 0, peer)

    def grad_copy(c, peer):
        return strip_copy(grad_out.at[c, peer], grad_in.at[c, strip], 1 + c, peer)

    def wide_copy(c, peer):
        part = wide.at[c, rows_of(strip), :]
        return strip_copy(part, part, 1 + chunks + c, peer)

    def mixed_copy(c, owner, peer):
        return strip_copy(
            mixed_out.at[c, rows_of(owner), :], mixed_in.at[c, strip, rows_of(owner), :],
            1 + 2 * chunks + c, peer,
        )

    def strip_all(ref, stage):
        return strip_copy(ref.at[mates], ref.at[mates], stage, strip)

    def wide_all(c):
        part = wide.at[c, pl.ds(0, (strips - 1) * columns), :]
        return strip_copy(part, part, 1 + chunks + c, strip)

    loads["field"].wait()
    for c in range(chunks):
        own = field[pl.ds(c, columns, stride=chunks), :]
        field_out[c] = own.astype(jnp.bfloat16)
        whole_field[c, rows_of(strip), :] = own
    pl.semaphore_wait(barrier, len(ang_peers) + len(strip_peers))
    for peer in strip_peers:
        field_copy(peer).start()
    loads["volume"].wait()
    pixels = volume.shape[0] // 2
    volume_half = both_parts(volume, pixels).astype(jnp.bfloat16)
    loads["radon"].wait()
    groups = 1 if angles & (angles - 1) or angles == 1 else 2
    members = angles // groups

    def project(group):
        first = pl.multiple_of(group * members * hit_rows, hit_rows)
        sums = dot(radon[pl.ds(first, members * hit_rows), :], volume_half).astype(jnp.bfloat16)
        for c in range(chunks):
            ray_out[c, pl.ds(group * members, members)] = (
                sums[:, c * slices:(c + 1) * slices].reshape(members, hit_rows, slices)
            )

    def start_rays(c, peers):
        for peer in peers:
            ray_copy(c, peer).start()

    mine = me // members
    for k in range(groups - 1, -1, -1):
        project(lax.rem(mine + k, groups))
        start_rays(0, ang_peers[:members] if k else ang_peers[(groups - 1) * members:])
    for c in range(chunks):
        for p in range(angles + 1):
            ray_in[c][pl.ds(p * detector, slack), :] = jnp.zeros((slack, slices), jnp.bfloat16)
        ray_in[c][window(me), :] = ray_out[c, me]
        for j in range(frames + 1):
            grads[c, pl.ds(j * (gap + side), gap), :] = jnp.zeros((gap, slices), jnp.float32)
    turned_radon[...] = radon[...].T
    for name in ("positions", "ranges", "tables", "probe", "measured", "dual"):
        loads[name].wait()
    cos_high, cos_low, sin_high, sin_low = (tables[k] for k in range(4))
    turn = tuple(
        above(beside(c, -s), beside(s, c)) for c, s in ((cos_high, sin_high), (cos_low, sin_low))
    )
    back_turn = tuple(
        above(beside(c, s), beside(-s, c)) for c, s in ((cos_high, sin_high), (cos_low, sin_low))
    )
    probe_re, probe_im = probe[0], probe[1]
    ray_weight = penalty - penalty * penalty * object_step
    grad_weight = penalty * object_step
    dual_weight = 1.0 - penalty * object_step
    for c in range(chunks):
        part = pl.ds(c, columns, stride=chunks)
        wide[c, rows_of(strip), :] = dual_weight * dual[part, :] + ray_weight * field[part, :]
    strip_all(field_in, 0).wait_recv()
    for c in range(chunks):
        for peer in strip_peers:
            wide_copy(c, peer).start()
    for peer in strip_peers:
        for c in range(chunks):
            whole_field[c, rows_of(peer), :] = field_in[peer, c].astype(jnp.float32)

    def frame_pair(pair):
        waves = []
        for j in (pair, pair + 1):
            re = whole_field[0, pl.ds(positions[j], side), :]
            im = whole_field[1, pl.ds(positions[j], side), :]
            waves.append(beside(probe_re * re - probe_im * im, probe_re * im + probe_im * re))
        right = dot3(split(above(*waves)), turn)
        far = dot3(back_turn, split(swap_blocks(right)))
        far_re, far_im = far[:side], far[side:]
        modulus = jnp.sqrt(far_re * far_re + far_im * far_im)
        intensity = beside(measured[pair], measured[pair + 1])
        shrink = 1.0 - jnp.sqrt(intensity) / jnp.maximum(modulus, 1.0)
        left = dot3(turn, split(above(far_re * shrink, far_im * shrink)))
        back = dot3(split(swap_blocks(left)), back_turn)
        for k in range(2):
            part = back[k * side:(k + 1) * side]
            re, im = part[:, :side], part[:, side:]
            rows = pl.ds(gap + (pair + k) * (gap + side), side)
            grads[0, rows, :] = probe_re * re + probe_im * im
            grads[1, rows, :] = probe_re * im - probe_im * re

    def deposit(c, first, rows):
        total = None
        for j in range(frames):
            start = gap + j * (gap + side) + first - positions[j]
            piece = grads[c, pl.ds(start, rows), :]
            total = piece if total is None else total + piece
        return total

    def sum_tile(c, tile):
        total = None
        for p in range(angles):
            start = ((slack + p * detector) // RAYS + tile - ranges[p]) * RAYS
            piece = ray_in[c][pl.ds(start, RAYS), :].astype(jnp.float32)
            total = piece if total is None else total + piece
        return total

    tiles = columns // RAYS
    def tile_rows(k):
        return pl.ds(k * RAYS, RAYS)

    def send_mixed(c):
        ray_all(c).wait_recv()
        for owner in [*strip_peers, strip]:
            for k in range(tiles):
                rays = sum_tile(c, owner * tiles + k)
                grad = deposit(c, owner * columns + k * RAYS, RAYS)
                mixed = ray_weight * rays + grad_weight * grad
                rows = pl.ds(pl.multiple_of(owner * columns + k * RAYS, RAYS), RAYS)
                own_mixed[c, rows, :] = mixed
                mixed_out[c, rows, :] = mixed.astype(jnp.bfloat16)
                if owner is strip:
                    own_rays[c, tile_rows(k), :] = rays
                    own_grad[c, tile_rows(k), :] = grad
                else:
                    grad_out[c, owner, tile_rows(k), :] = grad.astype(jnp.bfloat16)
            for peer in strip_peers:
                mixed_copy(c, owner, peer).start()

    def make_residual(c):
        wide_all(c).wait_recv()
        strip_all(mixed_in.at[c], 1 + 2 * chunks + c).wait_recv()
        for k in range(detector // RAYS):
            residual = own_mixed[c, tile_rows(k), :] - wide[c, tile_rows(k), :]
            for peer in strip_peers:
                residual = residual + mixed_in[c, peer, tile_rows(k), :].astype(jnp.float32)
            rows_half[c][tile_rows(k), :] = residual.astype(jnp.bfloat16)

    def send_parts(c):
        for peer in strip_peers:
            grad_copy(c, peer).start()

    def update(c):
        strip_all(grad_in.at[c], 1 + c).wait_recv()
        for k in range(tiles):
            here = tile_rows(k)
            own_tile = pl.ds(pl.multiple_of(strip * columns + k * RAYS, RAYS), RAYS)
            intersection, projection = own_grad[c, here, :], own_rays[c, here, :]
            for peer in strip_peers:
                grad = grad_in[c, peer, here, :].astype(jnp.float32)
                mixed = mixed_in[c, peer, own_tile, :].astype(jnp.float32)
                intersection = intersection + grad
                projection = projection + (mixed - grad_weight * grad) * (1.0 / ray_weight)
            part = pl.ds(c + k * RAYS * chunks, RAYS, stride=chunks)
            part_field, part_dual = field[part, :], dual[part, :]
            updated = part_field - object_step * (
                intersection + part_dual + penalty * (part_field - projection)
            )
            object_next[part, :] = updated
            dual_next[part, :] = part_dual + penalty * (updated - projection)

    def send_picks(c):
        make_residual(c)
        for peer in ang_peers:
            pick_out[c, peer] = rows_half[c][pl.ds(ranges[peer] * RAYS, hit_rows), :]
            pick_copy(c, peer).start()
        pick_in[c, me] = rows_half[c][pl.ds(ranges[me] * RAYS, hit_rows), :]

    for pair in range(0, frames, 2):
        frame_pair(pair)
        if pair == 2:
            for c in range(1, chunks):
                start_rays(c, ang_peers)
    for c in range(chunks):
        send_mixed(c)
        send_picks(c)
    for c in range(chunks):
        send_parts(c)
    for c in range(chunks):
        update(c)
    for c in range(chunks):
        pick_all(c).wait_recv()
        gradient = dot(turned_radon[...], pick_in[c].reshape(angles * hit_rows, slices))
        part = pl.ds(c, pixels, stride=chunks)
        volume_next[part, :] = volume[part, :] - volume_step * gradient
    for peer in strip_peers:
        field_copy(peer).wait_send()
    for c in range(chunks):
        ray_all(c).wait_send()
        pick_all(c).wait_send()
        strip_all(grad_out.at[c], 1 + c).wait_send()
        strip_all(mixed_in.at[c], 1 + 2 * chunks + c).wait_send()
        for peer in strip_peers:
            wide_copy(c, peer).wait_send()


def finish(first, second, third, first_out, second_out, third_out, sem):
    copies = [
        pltpu.make_async_copy(source, target, sem.at[k])
        for k, (source, target) in enumerate(
            ((first, first_out), (second, second_out), (third, third_out))
        )
    ]
    for copy in copies:
        copy.start()
    for copy in copies:
        copy.wait()


def body(
    measured, positions, probe_field, object_field, dual_field, volume, radon_tiles, tile_range
):
    angles, strips = lax.axis_size("ang"), lax.axis_size("strip")
    frames, side = measured.shape[1], measured.shape[2]
    columns = object_field.shape[1]
    hit_rows = radon_tiles.shape[2] * radon_tiles.shape[3]
    pixels = radon_tiles.shape[4]
    chunks, slices = object_field.shape[2], object_field.shape[3]
    detector = strips * columns
    pad_rows = detector - side + frames * detector
    half = jnp.bfloat16
    outs = pl.pallas_call(
        functools.partial(kernel, angles, strips),
        out_shape=(
            pltpu.VMEM((chunks * columns, slices), jnp.float32),
            pltpu.VMEM((chunks * columns, slices), jnp.float32),
            pltpu.VMEM((chunks * pixels, slices), jnp.float32),
        ),
        in_specs=[pl.BlockSpec(memory_space=pltpu.HBM)] * 9,
        out_specs=(pl.BlockSpec(memory_space=pltpu.VMEM),) * 3,
        scratch_shapes=[
            pltpu.SMEM((frames,), jnp.int32),
            pltpu.SMEM((angles,), jnp.int32),
            pltpu.VMEM((frames, side, side), jnp.float32),
            pltpu.VMEM((chunks, side, side), jnp.float32),
            pltpu.VMEM((chunks * columns, slices), jnp.float32),
            pltpu.VMEM((chunks * columns, slices), jnp.float32),
            pltpu.VMEM((chunks * pixels, slices), jnp.float32),
            pltpu.VMEM((angles * hit_rows, pixels), half),
            pltpu.VMEM((4, side, side), half),
            pltpu.VMEM((chunks, angles, hit_rows, slices), half),
            [pltpu.VMEM(((angles + 1) * detector - hit_rows, slices), half)] * chunks,
            pltpu.VMEM((chunks, angles, hit_rows, slices), half),
            pltpu.VMEM((chunks, angles, hit_rows, slices), half),
            pltpu.VMEM((chunks, columns, slices), half),
            pltpu.VMEM((strips, chunks, columns, slices), half),
        ] + [pltpu.VMEM((chunks, strips, columns, slices), half)] * 2 + [
            pltpu.VMEM((chunks, detector, slices), half),
            pltpu.VMEM((chunks, strips, detector, slices), half),
            pltpu.VMEM((chunks, detector, slices), jnp.float32),
            [pltpu.VMEM((detector, slices), half)] * chunks,
            pltpu.VMEM((chunks, detector, slices), jnp.float32),
            pltpu.VMEM((chunks, pad_rows, slices), jnp.float32),
            pltpu.VMEM((chunks, columns, slices), jnp.float32),
            pltpu.VMEM((chunks, columns, slices), jnp.float32),
            pltpu.VMEM((chunks, detector, slices), jnp.float32),
            pltpu.VMEM((pixels, angles * hit_rows), half),
            pltpu.SemaphoreType.DMA((9,)),
        ] + [pltpu.SemaphoreType.DMA((chunks,))] * 4
        + [pltpu.SemaphoreType.DMA((1 + 3 * chunks,))] * 2,
        compiler_params=pltpu.CompilerParams(
            collective_id=0, has_side_effects=True, vmem_limit_bytes=VMEM_BYTES
        ),
    )(
        positions.reshape(frames),
        tile_range.reshape(angles),
        measured[0],
        probe_field,
        object_field.reshape(chunks * columns, slices),
        dual_field.reshape(chunks * columns, slices),
        volume.reshape(chunks * pixels, slices),
        radon_tiles.reshape(angles * hit_rows, pixels),
        jnp.asarray(dft_tables(side)),
    )
    outs = pl.pallas_call(
        finish,
        out_shape=[jax.ShapeDtypeStruct(o.shape, o.dtype) for o in outs],
        in_specs=[pl.BlockSpec(memory_space=pl.ANY)] * 3,
        out_specs=[pl.BlockSpec(memory_space=pl.ANY)] * 3,
        scratch_shapes=[pltpu.SemaphoreType.DMA((3,))],
        compiler_params=pltpu.CompilerParams(vmem_limit_bytes=2 * 1024 * 1024),
    )(*outs)
    return (
        outs[0].reshape(object_field.shape),
        outs[1].reshape(dual_field.shape),
        outs[2].reshape(volume.shape),
    )


def solution(mesh):
    return jax.shard_map(
        body,
        mesh=mesh,
        in_specs=(
            P("ang", "strip", None, None),
            P("ang", "strip"),
            P(),
            P("ang", "strip", None, None),
            P("ang", "strip", None, None),
            P(("ang", "strip"), None, None),
            P(("ang", "strip"), None, None, None, None),
            P("ang", None, "strip", None),
        ),
        out_specs=(
            P("ang", "strip", None, None),
            P("ang", "strip", None, None),
            P(("ang", "strip"), None, None),
        ),
        check_vma=False,
    )
```

```python
import functools
import math

import jax
import jax.numpy as jnp
import numpy as np
from jax import lax
from jax.experimental import pallas as pl
from jax.experimental.pallas import tpu as pltpu
from jax.sharding import PartitionSpec as P

RAYS = 32
BLOCK = 128
VMEM_BYTES = 67043328 - 2 * 1024 * 1024

penalty = 1.0
object_step = 0.1
volume_step = 1.0
MESH = pl.DeviceIdType.MESH


def dft_tables(length):
    indices = np.arange(length, dtype=np.int64)
    angles = (indices[:, None] * indices[None, :] % length) * (2.0 * math.pi / length)
    scaling = 1.0 / math.sqrt(length)
    parts = []
    for table in (np.cos(angles) * scaling, np.sin(angles) * scaling):
        table = table.astype(np.float32)
        high = table.astype(jnp.bfloat16)
        parts += [high, (table - high.astype(np.float32)).astype(jnp.bfloat16)]
    return np.stack(parts)


def split(value):
    high = value.astype(jnp.bfloat16)
    return high, (value - high.astype(jnp.float32)).astype(jnp.bfloat16)


def dot(left, right):
    return jnp.dot(left, right, preferred_element_type=jnp.float32)


def dot3(left, right):
    return dot(
        jnp.concatenate([left[0], left[0], left[1]], axis=1),
        jnp.concatenate([right[0], right[1], right[0]], axis=0),
    )


def beside(left, right):
    return jnp.concatenate([left, right], axis=1)


def above(top, low):
    return jnp.concatenate([top, low], axis=0)


def swap_blocks(value):
    half = value.shape[1] // 2
    return above(
        beside(value[:half, :half], value[half:, :half]),
        beside(value[:half, half:], value[half:, half:]),
    )


def both_parts(ref, columns):
    return beside(ref[pl.ds(0, columns, stride=2), :], ref[pl.ds(1, columns, stride=2), :])


def xor(left, right, bound):
    result, bit = 0, 1
    while bit < bound:
        result = result + ((left // bit) + (right // bit)) % 2 * bit
        bit *= 2
    return result


def kernel(
    angles, strips,
    positions_hbm, ranges_hbm, measured_hbm, probe_hbm, field_hbm, dual_hbm, volume_hbm, radon_hbm,
    tables_hbm,
    object_next, dual_next, volume_next,
    positions, ranges, measured, probe, field, dual, volume, radon, tables,
    ray_out, ray_in, pick_out, pick_in, field_out, field_in, grad_out, grad_in,
    mixed_out, mixed_in, wide, rows_half, whole_field, grads,
    own_grad, own_rays, own_mixed, turned_radon,
    load_sem, ray_send, ray_recv, pick_send, pick_recv, strip_send, strip_recv,
):
    loads = {}
    for k, (name, source, target) in enumerate((
        ("field", field_hbm, field), ("volume", volume_hbm, volume), ("radon", radon_hbm, radon),
        ("positions", positions_hbm, positions), ("ranges", ranges_hbm, ranges),
        ("tables", tables_hbm, tables), ("probe", probe_hbm, probe),
        ("measured", measured_hbm, measured), ("dual", dual_hbm, dual),
    )):
        loads[name] = pltpu.make_async_copy(source, target, load_sem.at[k])
        loads[name].start()
    me, strip = lax.axis_index("ang"), lax.axis_index("strip")
    columns = field.shape[0] // 2
    detector = strips * columns
    frames, side = measured.shape[0], measured.shape[1]
    slices = field.shape[1]
    chunks, hit_rows = ray_out.shape[0], ray_out.shape[2]
    gap = detector - side
    if angles & (angles - 1) or angles < 4:
        groups, members, edge = 1, angles, me >= 0
        ang_peers = [lax.rem(me + offset, angles) for offset in range(1, angles)]
        far_peers = []
    else:
        groups, members, quarter = 2, angles // 2, angles // 4
        plane, low = me // quarter, lax.rem(me, quarter)
        side_of = me // members
        edge = (plane + 1) // 2 * 2 != 2
        mates = [xor(low, j, quarter) for j in range(quarter - 1, -1, -1)]
        ang_peers = [
            there * quarter + mate
            for there in (3 - 3 * side_of, 2 - side_of, 4 * side_of + 1 - plane)
            for mate in mates
        ] + [plane * quarter + mate for mate in mates[:-1]]
        far_peers = ang_peers[:members]
    near_peers = ang_peers[len(far_peers):]
    strip_peers = [lax.rem(strip + offset, strips) for offset in range(1, strips)]

    def rows_of(owner):
        return pl.ds(pl.multiple_of(owner * columns, columns), columns)

    barrier = pltpu.get_barrier_semaphore()
    for peer in ang_peers:
        pl.semaphore_signal(barrier, inc=1, device_id=(peer, strip), device_id_type=MESH)
    for peer in strip_peers:
        pl.semaphore_signal(barrier, inc=1, device_id=(me, peer), device_id_type=MESH)

    def remote(source, target, send, recv, device):
        return pltpu.make_async_remote_copy(
            src_ref=source, dst_ref=target, send_sem=send, recv_sem=recv,
            device_id=device, device_id_type=MESH,
        )

    others = pl.ds(0, angles - 1)
    slack = detector - hit_rows

    def window(slot):
        return pl.ds(pl.multiple_of(slack + slot * detector, RAYS), hit_rows)

    rest = pl.ds(0, strips - 1)

    def ray_copy(c, peer):
        return remote(
            ray_out.at[c, peer], ray_in[c].at[window(me)], ray_send.at[c], ray_recv.at[c],
            (peer, strip),
        )

    def ray_all(c):
        part = ray_in[c].at[pl.ds(0, (angles - 1) * hit_rows)]
        return remote(part, part, ray_send.at[c], ray_recv.at[c], (me, strip))

    def pick_copy(c, peer):
        return remote(
            pick_out.at[c, peer], pick_in.at[c, me], pick_send.at[c], pick_recv.at[c],
            (peer, strip),
        )

    def pick_all(c):
        return remote(
            pick_out.at[c, others], pick_in.at[c, others], pick_send.at[c], pick_recv.at[c],
            (me, strip),
        )

    def strip_copy(source, target, stage, peer):
        return remote(source, target, strip_send.at[stage], strip_recv.at[stage], (me, peer))

    def field_copy(peer):
        return strip_copy(field_out, field_in.at[strip], 0, peer)

    def grad_copy(c, peer):
        return strip_copy(grad_out.at[c, peer], grad_in.at[c, strip], 1 + c, peer)

    def wide_copy(c, peer):
        part = wide.at[c, rows_of(strip), :]
        return strip_copy(part, part, 1 + chunks + c, peer)

    def mixed_copy(c, owner, peer):
        return strip_copy(
            mixed_out.at[c, rows_of(owner), :], mixed_in.at[c, strip, rows_of(owner), :],
            1 + 2 * chunks + c, peer,
        )

    def strip_all(ref, stage):
        return strip_copy(ref.at[rest], ref.at[rest], stage, strip)

    def wide_all(c):
        part = wide.at[c, pl.ds(0, (strips - 1) * columns), :]
        return strip_copy(part, part, 1 + chunks + c, strip)

    loads["field"].wait()
    for c in range(chunks):
        own = field[pl.ds(c, columns, stride=chunks), :]
        field_out[c] = own.astype(jnp.bfloat16)
        whole_field[c, rows_of(strip), :] = own
    loads["volume"].wait()
    pixels = volume.shape[0] // 2
    volume_half = both_parts(volume, pixels).astype(jnp.bfloat16)
    loads["radon"].wait()
    def project(group):
        first = pl.multiple_of(group * members * hit_rows, hit_rows)
        sums = dot(radon[pl.ds(first, members * hit_rows), :], volume_half).astype(jnp.bfloat16)
        for c in range(chunks):
            ray_out[c, pl.ds(group * members, members)] = (
                sums[:, c * slices:(c + 1) * slices].reshape(members, hit_rows, slices)
            )

    def start_rays(c, peers):
        for peer in peers:
            ray_copy(c, peer).start()

    mine = me // members
    project(lax.rem(mine + groups - 1, groups))
    pl.semaphore_wait(barrier, len(ang_peers) + len(strip_peers))
    for peer in strip_peers:
        field_copy(peer).start()
    start_rays(0, far_peers)
    if groups > 1:
        project(mine)
    start_rays(0, near_peers)

    @pl.when(jnp.logical_not(edge))
    def _():
        for c in range(1, chunks):
            start_rays(c, ang_peers)

    for c in range(chunks):
        for p in range(angles + 1):
            ray_in[c][pl.ds(p * detector, slack), :] = jnp.zeros((slack, slices), jnp.bfloat16)
        ray_in[c][window(me), :] = ray_out[c, me]
        for j in range(frames + 1):
            grads[c, pl.ds(j * (gap + side), gap), :] = jnp.zeros((gap, slices), jnp.float32)
    turned_radon[...] = radon[...].T
    for name in ("positions", "ranges", "tables", "probe", "measured", "dual"):
        loads[name].wait()
    cos_high, cos_low, sin_high, sin_low = (tables[k] for k in range(4))
    turn = tuple(
        above(beside(c, -s), beside(s, c)) for c, s in ((cos_high, sin_high), (cos_low, sin_low))
    )
    back_turn = tuple(
        above(beside(c, s), beside(-s, c)) for c, s in ((cos_high, sin_high), (cos_low, sin_low))
    )
    probe_re, probe_im = probe[0], probe[1]
    ray_weight = penalty - penalty * penalty * object_step
    grad_weight = penalty * object_step
    dual_weight = 1.0 - penalty * object_step
    for c in range(chunks):
        part = pl.ds(c, columns, stride=chunks)
        wide[c, rows_of(strip), :] = dual_weight * dual[part, :] + ray_weight * field[part, :]
    strip_all(field_in, 0).wait_recv()
    for c in range(chunks):
        for peer in strip_peers:
            wide_copy(c, peer).start()
    for peer in strip_peers:
        for c in range(chunks):
            whole_field[c, rows_of(peer), :] = field_in[peer, c].astype(jnp.float32)

    def frame_pair(pair):
        waves = []
        for j in (pair, pair + 1):
            re = whole_field[0, pl.ds(positions[j], side), :]
            im = whole_field[1, pl.ds(positions[j], side), :]
            waves.append(beside(probe_re * re - probe_im * im, probe_re * im + probe_im * re))
        right = dot3(split(above(*waves)), turn)
        far = dot3(back_turn, split(swap_blocks(right)))
        far_re, far_im = far[:side], far[side:]
        modulus = jnp.sqrt(far_re * far_re + far_im * far_im)
        intensity = beside(measured[pair], measured[pair + 1])
        shrink = 1.0 - jnp.sqrt(intensity) / jnp.maximum(modulus, 1.0)
        left = dot3(turn, split(above(far_re * shrink, far_im * shrink)))
        back = dot3(split(swap_blocks(left)), back_turn)
        for k in range(2):
            part = back[k * side:(k + 1) * side]
            re, im = part[:, :side], part[:, side:]
            rows = pl.ds(gap + (pair + k) * (gap + side), side)
            grads[0, rows, :] = probe_re * re + probe_im * im
            grads[1, rows, :] = probe_re * im - probe_im * re

    def deposit(c, first, rows):
        total = None
        for j in range(frames):
            start = gap + j * (gap + side) + first - positions[j]
            piece = grads[c, pl.ds(start, rows), :]
            total = piece if total is None else total + piece
        return total

    def sum_rays(c, first, rows):
        total = None
        for p in range(angles):
            start = ((slack + p * detector + first) // RAYS - ranges[p]) * RAYS
            piece = ray_in[c][pl.ds(start, rows), :].astype(jnp.float32)
            total = piece if total is None else total + piece
        return total

    tiles, block = columns // RAYS, math.gcd(BLOCK, columns)

    def tile_rows(k):
        return pl.ds(k * RAYS, RAYS)

    def send_mixed(c):
        ray_all(c).wait_recv()
        for owner in [*strip_peers, strip]:
            for k in range(0, columns, block):
                first = pl.multiple_of(owner * columns + k, block)
                rays = sum_rays(c, first, block)
                grad = deposit(c, first, block)
                mixed = ray_weight * rays + grad_weight * grad
                own_mixed[c, pl.ds(first, block), :] = mixed
                mixed_out[c, pl.ds(first, block), :] = mixed.astype(jnp.bfloat16)
                if owner is strip:
                    own_rays[c, pl.ds(k, block), :] = rays
                    own_grad[c, pl.ds(k, block), :] = grad
                else:
                    grad_out[c, owner, pl.ds(k, block), :] = grad.astype(jnp.bfloat16)
            for peer in strip_peers:
                mixed_copy(c, owner, peer).start()

    def make_residual(c):
        wide_all(c).wait_recv()
        strip_all(mixed_in.at[c], 1 + 2 * chunks + c).wait_recv()
        for k in range(detector // RAYS):
            residual = own_mixed[c, tile_rows(k), :] - wide[c, tile_rows(k), :]
            for peer in strip_peers:
                residual = residual + mixed_in[c, peer, tile_rows(k), :].astype(jnp.float32)
            rows_half[c][tile_rows(k), :] = residual.astype(jnp.bfloat16)

    def send_parts(c):
        for peer in strip_peers:
            grad_copy(c, peer).start()

    def update(c):
        strip_all(grad_in.at[c], 1 + c).wait_recv()
        for k in range(tiles):
            here = tile_rows(k)
            own_tile = pl.ds(pl.multiple_of(strip * columns + k * RAYS, RAYS), RAYS)
            intersection, projection = own_grad[c, here, :], own_rays[c, here, :]
            for peer in strip_peers:
                grad = grad_in[c, peer, here, :].astype(jnp.float32)
                mixed = mixed_in[c, peer, own_tile, :].astype(jnp.float32)
                intersection = intersection + grad
                projection = projection + (mixed - grad_weight * grad) * (1.0 / ray_weight)
            part = pl.ds(c + k * RAYS * chunks, RAYS, stride=chunks)
            part_field, part_dual = field[part, :], dual[part, :]
            updated = part_field - object_step * (
                intersection + part_dual + penalty * (part_field - projection)
            )
            object_next[part, :] = updated
            dual_next[part, :] = part_dual + penalty * (updated - projection)

    def send_picks(c):
        make_residual(c)
        for peer in ang_peers:
            pick_out[c, peer] = rows_half[c][pl.ds(ranges[peer] * RAYS, hit_rows), :]
            pick_copy(c, peer).start()
        pick_in[c, me] = rows_half[c][pl.ds(ranges[me] * RAYS, hit_rows), :]

    for pair in range(0, frames, 2):
        frame_pair(pair)
        if pair == 0:

            @pl.when(edge)
            def _():
                for c in range(1, chunks):
                    start_rays(c, ang_peers)

    for c in range(chunks):
        send_mixed(c)
        send_picks(c)
    for c in range(chunks):
        send_parts(c)
    for c in range(chunks):
        update(c)
    for c in range(chunks):
        pick_all(c).wait_recv()
        gradient = dot(turned_radon[...], pick_in[c].reshape(angles * hit_rows, slices))
        part = pl.ds(c, pixels, stride=chunks)
        volume_next[part, :] = volume[part, :] - volume_step * gradient
    for peer in strip_peers:
        field_copy(peer).wait_send()
    for c in range(chunks):
        ray_all(c).wait_send()
        pick_all(c).wait_send()
        strip_all(grad_out.at[c], 1 + c).wait_send()
        strip_all(mixed_in.at[c], 1 + 2 * chunks + c).wait_send()
        for peer in strip_peers:
            wide_copy(c, peer).wait_send()


def finish(first, second, third, first_out, second_out, third_out, sem):
    copies = [
        pltpu.make_async_copy(source, target, sem.at[k])
        for k, (source, target) in enumerate(
            ((first, first_out), (second, second_out), (third, third_out))
        )
    ]
    for copy in copies:
        copy.start()
    for copy in copies:
        copy.wait()


def body(
    measured, positions, probe_field, object_field, dual_field, volume, radon_tiles, tile_range
):
    angles, strips = lax.axis_size("ang"), lax.axis_size("strip")
    frames, side = measured.shape[1], measured.shape[2]
    columns = object_field.shape[1]
    hit_rows = radon_tiles.shape[2] * radon_tiles.shape[3]
    pixels = radon_tiles.shape[4]
    chunks, slices = object_field.shape[2], object_field.shape[3]
    detector = strips * columns
    pad_rows = detector - side + frames * detector
    half = jnp.bfloat16
    outs = pl.pallas_call(
        functools.partial(kernel, angles, strips),
        out_shape=(
            pltpu.VMEM((chunks * columns, slices), jnp.float32),
            pltpu.VMEM((chunks * columns, slices), jnp.float32),
            pltpu.VMEM((chunks * pixels, slices), jnp.float32),
        ),
        in_specs=[pl.BlockSpec(memory_space=pltpu.HBM)] * 9,
        out_specs=(pl.BlockSpec(memory_space=pltpu.VMEM),) * 3,
        scratch_shapes=[
            pltpu.SMEM((frames,), jnp.int32),
            pltpu.SMEM((angles,), jnp.int32),
            pltpu.VMEM((frames, side, side), jnp.float32),
            pltpu.VMEM((chunks, side, side), jnp.float32),
            pltpu.VMEM((chunks * columns, slices), jnp.float32),
            pltpu.VMEM((chunks * columns, slices), jnp.float32),
            pltpu.VMEM((chunks * pixels, slices), jnp.float32),
            pltpu.VMEM((angles * hit_rows, pixels), half),
            pltpu.VMEM((4, side, side), half),
            pltpu.VMEM((chunks, angles, hit_rows, slices), half),
            [pltpu.VMEM(((angles + 1) * detector - hit_rows, slices), half)] * chunks,
            pltpu.VMEM((chunks, angles, hit_rows, slices), half),
            pltpu.VMEM((chunks, angles, hit_rows, slices), half),
            pltpu.VMEM((chunks, columns, slices), half),
            pltpu.VMEM((strips, chunks, columns, slices), half),
        ] + [pltpu.VMEM((chunks, strips, columns, slices), half)] * 2 + [
            pltpu.VMEM((chunks, detector, slices), half),
            pltpu.VMEM((chunks, strips, detector, slices), half),
            pltpu.VMEM((chunks, detector, slices), jnp.float32),
            [pltpu.VMEM((detector, slices), half)] * chunks,
            pltpu.VMEM((chunks, detector, slices), jnp.float32),
            pltpu.VMEM((chunks, pad_rows, slices), jnp.float32),
            pltpu.VMEM((chunks, columns, slices), jnp.float32),
            pltpu.VMEM((chunks, columns, slices), jnp.float32),
            pltpu.VMEM((chunks, detector, slices), jnp.float32),
            pltpu.VMEM((pixels, angles * hit_rows), half),
            pltpu.SemaphoreType.DMA((9,)),
        ] + [pltpu.SemaphoreType.DMA((chunks,))] * 4
        + [pltpu.SemaphoreType.DMA((1 + 3 * chunks,))] * 2,
        compiler_params=pltpu.CompilerParams(
            collective_id=0, has_side_effects=True, vmem_limit_bytes=VMEM_BYTES
        ),
    )(
        positions.reshape(frames),
        tile_range.reshape(angles),
        measured[0],
        probe_field,
        object_field.reshape(chunks * columns, slices),
        dual_field.reshape(chunks * columns, slices),
        volume.reshape(chunks * pixels, slices),
        radon_tiles.reshape(angles * hit_rows, pixels),
        jnp.asarray(dft_tables(side)),
    )
    outs = pl.pallas_call(
        finish,
        out_shape=[jax.ShapeDtypeStruct(o.shape, o.dtype) for o in outs],
        in_specs=[pl.BlockSpec(memory_space=pl.ANY)] * 3,
        out_specs=[pl.BlockSpec(memory_space=pl.ANY)] * 3,
        scratch_shapes=[pltpu.SemaphoreType.DMA((3,))],
        compiler_params=pltpu.CompilerParams(vmem_limit_bytes=2 * 1024 * 1024),
    )(*outs)
    return (
        outs[0].reshape(object_field.shape),
        outs[1].reshape(dual_field.shape),
        outs[2].reshape(volume.shape),
    )


def solution(mesh):
    return jax.shard_map(
        body,
        mesh=mesh,
        in_specs=(
            P("ang", "strip", None, None),
            P("ang", "strip"),
            P(),
            P("ang", "strip", None, None),
            P("ang", "strip", None, None),
            P(("ang", "strip"), None, None),
            P(("ang", "strip"), None, None, None, None),
            P("ang", None, "strip", None),
        ),
        out_specs=(
            P("ang", "strip", None, None),
            P("ang", "strip", None, None),
            P(("ang", "strip"), None, None),
        ),
        check_vma=False,
    )
```

```python
import functools
import math

import jax
import jax.numpy as jnp
import numpy as np
from jax import lax
from jax.experimental import pallas as pl
from jax.experimental.pallas import tpu as pltpu
from jax.sharding import PartitionSpec as P

RAYS = 32
BLOCK = 128
VMEM_BYTES = 67043328 - 2 * 1024 * 1024

penalty = 1.0
object_step = 0.1
volume_step = 1.0
MESH = pl.DeviceIdType.MESH


def dft_tables(length):
    indices = np.arange(length, dtype=np.int64)
    angles = (indices[:, None] * indices[None, :] % length) * (2.0 * math.pi / length)
    scaling = 1.0 / math.sqrt(length)
    parts = []
    for table in (np.cos(angles) * scaling, np.sin(angles) * scaling):
        table = table.astype(np.float32)
        high = table.astype(jnp.bfloat16)
        parts += [high, (table - high.astype(np.float32)).astype(jnp.bfloat16)]
    return np.stack(parts)


def split(value):
    high = value.astype(jnp.bfloat16)
    return high, (value - high.astype(jnp.float32)).astype(jnp.bfloat16)


def dot(left, right):
    return jnp.dot(left, right, preferred_element_type=jnp.float32)


def dot3(left, right):
    return dot(
        jnp.concatenate([left[0], left[0], left[1]], axis=1),
        jnp.concatenate([right[0], right[1], right[0]], axis=0),
    )


def dot2(left, right):
    return dot(jnp.concatenate([left[0], left[1]], axis=1), jnp.concatenate([right, right], axis=0))


def beside(left, right):
    return jnp.concatenate([left, right], axis=1)


def above(top, low):
    return jnp.concatenate([top, low], axis=0)


def swap_blocks(value):
    half = value.shape[1] // 2
    return above(
        beside(value[:half, :half], value[half:, :half]),
        beside(value[:half, half:], value[half:, half:]),
    )


def both_parts(ref, columns):
    return beside(ref[pl.ds(0, columns, stride=2), :], ref[pl.ds(1, columns, stride=2), :])


def xor(left, right, bound):
    result, bit = 0, 1
    while bit < bound:
        result = result + ((left // bit) + (right // bit)) % 2 * bit
        bit *= 2
    return result


def kernel(
    angles, strips,
    positions_hbm, ranges_hbm, measured_hbm, probe_hbm, field_hbm, dual_hbm, volume_hbm, radon_hbm,
    tables_hbm,
    object_next, dual_next, volume_next,
    positions, ranges, measured, probe, field, dual, volume, radon, tables,
    ray_out, ray_in, pick_out, pick_in, field_out, field_in, grad_out, grad_in,
    mixed_out, mixed_in, wide_out, wide_in, rows_half, whole_field, grads,
    own_grad, own_rays, own_mixed, turned_radon,
    load_sem, ray_send, ray_recv, pick_send, pick_recv, strip_send, strip_recv,
):
    loads = {}
    for k, (name, source, target) in enumerate((
        ("field", field_hbm, field), ("volume", volume_hbm, volume), ("radon", radon_hbm, radon),
        ("dual", dual_hbm, dual), ("positions", positions_hbm, positions), ("ranges", ranges_hbm, ranges),
        ("tables", tables_hbm, tables), ("probe", probe_hbm, probe),
        ("measured", measured_hbm, measured),
    )):
        loads[name] = pltpu.make_async_copy(source, target, load_sem.at[k])
        loads[name].start()
    me, strip = lax.axis_index("ang"), lax.axis_index("strip")
    columns = field.shape[0] // 2
    detector = strips * columns
    frames, side = measured.shape[0], measured.shape[1]
    slices = field.shape[1]
    chunks, hit_rows = ray_out.shape[0], ray_out.shape[2]
    gap = detector - side
    if angles & (angles - 1) or angles < 4:
        groups, members, edge = 1, angles, me >= 0
        ang_peers = [lax.rem(me + offset, angles) for offset in range(1, angles)]
        far_peers = []
    else:
        groups, members, quarter = 2, angles // 2, angles // 4
        plane, low = me // quarter, lax.rem(me, quarter)
        side_of = me // members
        edge = (plane + 1) // 2 * 2 != 2
        mates = [xor(low, j, quarter) for j in range(quarter - 1, -1, -1)]
        ang_peers = [
            there * quarter + mate
            for there in (3 - 3 * side_of, 2 - side_of, 4 * side_of + 1 - plane)
            for mate in mates
        ] + [plane * quarter + mate for mate in mates[:-1]]
        far_peers = ang_peers[:members]
    near_peers = ang_peers[len(far_peers):]
    strip_peers = [lax.rem(strip + offset, strips) for offset in range(1, strips)]

    def rows_of(owner):
        return pl.ds(pl.multiple_of(owner * columns, columns), columns)

    barrier = pltpu.get_barrier_semaphore()
    for peer in ang_peers:
        pl.semaphore_signal(barrier, inc=1, device_id=(peer, strip), device_id_type=MESH)
    for peer in strip_peers:
        pl.semaphore_signal(barrier, inc=1, device_id=(me, peer), device_id_type=MESH)

    def remote(source, target, send, recv, device):
        return pltpu.make_async_remote_copy(
            src_ref=source, dst_ref=target, send_sem=send, recv_sem=recv,
            device_id=device, device_id_type=MESH,
        )

    others = pl.ds(0, angles - 1)
    slack = detector - hit_rows

    def window(slot):
        return pl.ds(pl.multiple_of(slack + slot * detector, RAYS), hit_rows)

    rest = pl.ds(0, strips - 1)

    def ray_copy(c, peer):
        return remote(
            ray_out.at[c, peer], ray_in[c].at[window(me)], ray_send.at[c], ray_recv.at[c],
            (peer, strip),
        )

    def ray_all(c):
        part = ray_in[c].at[pl.ds(0, (angles - 1) * hit_rows)]
        return remote(part, part, ray_send.at[c], ray_recv.at[c], (me, strip))

    def pick_copy(c, peer):
        return remote(
            pick_out.at[c, peer], pick_in.at[c, me], pick_send.at[c], pick_recv.at[c],
            (peer, strip),
        )

    def pick_all(c):
        return remote(
            pick_out.at[c, others], pick_in.at[c, others], pick_send.at[c], pick_recv.at[c],
            (me, strip),
        )

    def strip_copy(source, target, stage, peer):
        return remote(source, target, strip_send.at[stage], strip_recv.at[stage], (me, peer))

    def field_copy(peer):
        return strip_copy(field_out, field_in.at[strip], 0, peer)

    def grad_copy(c, peer):
        return strip_copy(grad_out.at[c, peer], grad_in.at[c, strip], 1 + c, peer)

    def wide_copy(c, peer):
        return strip_copy(wide_out[c], wide_in[c].at[strip], 1 + chunks + c, peer)

    def mixed_copy(c, owner, peer):
        return strip_copy(
            mixed_out.at[c, rows_of(owner), :], mixed_in.at[c, strip, rows_of(owner), :],
            1 + 2 * chunks + c, peer,
        )

    def strip_all(ref, stage):
        return strip_copy(ref.at[rest], ref.at[rest], stage, strip)

    loads["field"].wait()
    for c in range(chunks):
        own = field[pl.ds(c, columns, stride=chunks), :]
        field_out[c] = own.astype(jnp.bfloat16)
        whole_field[c, rows_of(strip), :] = own
    loads["volume"].wait()
    pixels = volume.shape[0] // 2
    volume_half = both_parts(volume, pixels).astype(jnp.bfloat16)
    loads["radon"].wait()
    def project(group):
        first = pl.multiple_of(group * members * hit_rows, hit_rows)
        sums = dot(radon[pl.ds(first, members * hit_rows), :], volume_half).astype(jnp.bfloat16)
        for c in range(chunks):
            ray_out[c, pl.ds(group * members, members)] = (
                sums[:, c * slices:(c + 1) * slices].reshape(members, hit_rows, slices)
            )

    def start_rays(c, peers):
        for peer in peers:
            ray_copy(c, peer).start()

    mine = me // members
    project(lax.rem(mine + groups - 1, groups))
    loads["dual"].wait()
    ray_weight = penalty - penalty * penalty * object_step
    grad_weight = penalty * object_step
    dual_weight = 1.0 - penalty * object_step
    for c in range(chunks):
        part = pl.ds(c, columns, stride=chunks)
        below = field[part, :] - field_out[c].astype(jnp.float32)
        wide_out[c][...] = (dual_weight * dual[part, :] + ray_weight * below).astype(
            wide_out[c].dtype
        )
    pl.semaphore_wait(barrier, len(ang_peers) + len(strip_peers))
    for peer in strip_peers:
        field_copy(peer).start()
    start_rays(0, far_peers)
    if groups > 1:
        project(mine)
    start_rays(0, near_peers)
    for c in range(chunks):
        for peer in strip_peers:
            wide_copy(c, peer).start()

    @pl.when(jnp.logical_not(edge))
    def _():
        for c in range(1, chunks):
            start_rays(c, ang_peers)

    for c in range(chunks):
        for p in range(angles + 1):
            ray_in[c][pl.ds(p * detector, slack), :] = jnp.zeros((slack, slices), jnp.bfloat16)
        ray_in[c][window(me), :] = ray_out[c, me]
        for j in range(frames + 1):
            grads[c, pl.ds(j * (gap + side), gap), :] = jnp.zeros((gap, slices), jnp.float32)
    turned_radon[...] = radon[...].T
    for name in ("positions", "ranges", "tables", "probe", "measured"):
        loads[name].wait()
    cos_high, cos_low, sin_high, sin_low = (tables[k] for k in range(4))
    turn = tuple(
        above(beside(c, -s), beside(s, c)) for c, s in ((cos_high, sin_high), (cos_low, sin_low))
    )
    back_turn = tuple(
        above(beside(c, s), beside(-s, c)) for c, s in ((cos_high, sin_high), (cos_low, sin_low))
    )
    probe_re, probe_im = probe[0], probe[1]
    strip_all(field_in, 0).wait_recv()
    for peer in strip_peers:
        for c in range(chunks):
            whole_field[c, rows_of(peer), :] = field_in[peer, c].astype(jnp.float32)

    def frame_pair(pair):
        waves = []
        for j in (pair, pair + 1):
            re = whole_field[0, pl.ds(positions[j], side), :]
            im = whole_field[1, pl.ds(positions[j], side), :]
            waves.append(beside(probe_re * re - probe_im * im, probe_re * im + probe_im * re))
        right = dot3(split(above(*waves)), turn)
        far = dot3(back_turn, split(swap_blocks(right)))
        far_re, far_im = far[:side], far[side:]
        modulus = jnp.sqrt(far_re * far_re + far_im * far_im)
        intensity = beside(measured[pair], measured[pair + 1])
        shrink = 1.0 - jnp.sqrt(intensity) / jnp.maximum(modulus, 1.0)
        left = dot2(turn, above(far_re * shrink, far_im * shrink).astype(jnp.bfloat16))
        back = dot(
            beside(*[swap_blocks(left).astype(jnp.bfloat16)] * 2), above(*back_turn)
        )
        for k in range(2):
            part = back[k * side:(k + 1) * side]
            re, im = part[:, :side], part[:, side:]
            rows = pl.ds(gap + (pair + k) * (gap + side), side)
            grads[0, rows, :] = probe_re * re + probe_im * im
            grads[1, rows, :] = probe_re * im - probe_im * re

    def deposit(c, first, rows):
        total = None
        for j in range(frames):
            start = gap + j * (gap + side) + first - positions[j]
            piece = grads[c, pl.ds(start, rows), :]
            total = piece if total is None else total + piece
        return total

    def sum_rays(c, first, rows):
        total = None
        for p in range(angles):
            start = ((slack + p * detector + first) // RAYS - ranges[p]) * RAYS
            piece = ray_in[c][pl.ds(start, rows), :].astype(jnp.float32)
            total = piece if total is None else total + piece
        return total

    tiles, block = columns // RAYS, math.gcd(BLOCK, columns)

    def tile_rows(k):
        return pl.ds(k * RAYS, RAYS)

    def send_mixed(c):
        ray_all(c).wait_recv()
        for owner in [*strip_peers, strip]:
            for k in range(0, columns, block):
                first = pl.multiple_of(owner * columns + k, block)
                rays = sum_rays(c, first, block)
                grad = deposit(c, first, block)
                mixed = ray_weight * rays + grad_weight * grad
                own_mixed[c, pl.ds(first, block), :] = mixed
                mixed_out[c, pl.ds(first, block), :] = mixed.astype(jnp.bfloat16)
                if owner is strip:
                    own_rays[c, pl.ds(k, block), :] = rays
                    own_grad[c, pl.ds(k, block), :] = grad
                else:
                    grad_out[c, owner, pl.ds(k, block), :] = grad.astype(jnp.bfloat16)
            for peer in strip_peers:
                mixed_copy(c, owner, peer).start()

    def make_residual(c):
        strip_all(wide_in[c], 1 + chunks + c).wait_recv()
        strip_all(mixed_in.at[c], 1 + 2 * chunks + c).wait_recv()
        for owner in [*strip_peers, strip]:
            for k in range(tiles):
                rows = pl.ds(pl.multiple_of(owner * columns + k * RAYS, RAYS), RAYS)
                residual = own_mixed[c, rows, :] - ray_weight * whole_field[c, rows, :]
                if owner is strip:
                    part = pl.ds(c + k * RAYS * chunks, RAYS, stride=chunks)
                    residual = residual - dual_weight * dual[part, :]
                else:
                    residual = residual - wide_in[c][owner, tile_rows(k), :].astype(jnp.float32)
                for peer in strip_peers:
                    residual = residual + mixed_in[c, peer, rows, :].astype(jnp.float32)
                rows_half[c][rows, :] = residual.astype(jnp.bfloat16)

    def send_parts(c):
        for peer in strip_peers:
            grad_copy(c, peer).start()

    def update(c):
        strip_all(grad_in.at[c], 1 + c).wait_recv()
        for k in range(tiles):
            here = tile_rows(k)
            own_tile = pl.ds(pl.multiple_of(strip * columns + k * RAYS, RAYS), RAYS)
            intersection, projection = own_grad[c, here, :], own_rays[c, here, :]
            for peer in strip_peers:
                grad = grad_in[c, peer, here, :].astype(jnp.float32)
                mixed = mixed_in[c, peer, own_tile, :].astype(jnp.float32)
                intersection = intersection + grad
                projection = projection + (mixed - grad_weight * grad) * (1.0 / ray_weight)
            part = pl.ds(c + k * RAYS * chunks, RAYS, stride=chunks)
            part_field, part_dual = field[part, :], dual[part, :]
            updated = part_field - object_step * (
                intersection + part_dual + penalty * (part_field - projection)
            )
            object_next[part, :] = updated
            dual_next[part, :] = part_dual + penalty * (updated - projection)

    def send_picks(c):
        make_residual(c)
        for peer in ang_peers:
            pick_out[c, peer] = rows_half[c][pl.ds(ranges[peer] * RAYS, hit_rows), :]
            pick_copy(c, peer).start()
        pick_in[c, me] = rows_half[c][pl.ds(ranges[me] * RAYS, hit_rows), :]

    for pair in range(0, frames, 2):
        frame_pair(pair)
        if pair == 0:

            @pl.when(edge)
            def _():
                for c in range(1, chunks):
                    start_rays(c, ang_peers)

    for c in range(chunks):
        send_mixed(c)
        send_picks(c)
    for c in range(chunks):
        send_parts(c)
    for c in range(chunks):
        update(c)
    for c in range(chunks):
        pick_all(c).wait_recv()
        gradient = dot(turned_radon[...], pick_in[c].reshape(angles * hit_rows, slices))
        part = pl.ds(c, pixels, stride=chunks)
        volume_next[part, :] = volume[part, :] - volume_step * gradient
    for peer in strip_peers:
        field_copy(peer).wait_send()
    for c in range(chunks):
        ray_all(c).wait_send()
        pick_all(c).wait_send()
        strip_all(grad_out.at[c], 1 + c).wait_send()
        strip_all(mixed_in.at[c], 1 + 2 * chunks + c).wait_send()
        for peer in strip_peers:
            wide_copy(c, peer).wait_send()


def finish(first, second, third, first_out, second_out, third_out, sem):
    copies = [
        pltpu.make_async_copy(source, target, sem.at[k])
        for k, (source, target) in enumerate(
            ((first, first_out), (second, second_out), (third, third_out))
        )
    ]
    for copy in copies:
        copy.start()
    for copy in copies:
        copy.wait()


def body(
    measured, positions, probe_field, object_field, dual_field, volume, radon_tiles, tile_range
):
    angles, strips = lax.axis_size("ang"), lax.axis_size("strip")
    frames, side = measured.shape[1], measured.shape[2]
    columns = object_field.shape[1]
    hit_rows = radon_tiles.shape[2] * radon_tiles.shape[3]
    pixels = radon_tiles.shape[4]
    chunks, slices = object_field.shape[2], object_field.shape[3]
    detector = strips * columns
    pad_rows = detector - side + frames * detector
    half = jnp.bfloat16
    wide_kinds = [half] + [jnp.float32] * (chunks - 1)
    outs = pl.pallas_call(
        functools.partial(kernel, angles, strips),
        out_shape=(
            pltpu.VMEM((chunks * columns, slices), jnp.float32),
            pltpu.VMEM((chunks * columns, slices), jnp.float32),
            pltpu.VMEM((chunks * pixels, slices), jnp.float32),
        ),
        in_specs=[pl.BlockSpec(memory_space=pltpu.HBM)] * 9,
        out_specs=(pl.BlockSpec(memory_space=pltpu.VMEM),) * 3,
        scratch_shapes=[
            pltpu.SMEM((frames,), jnp.int32),
            pltpu.SMEM((angles,), jnp.int32),
            pltpu.VMEM((frames, side, side), jnp.float32),
            pltpu.VMEM((chunks, side, side), jnp.float32),
            pltpu.VMEM((chunks * columns, slices), jnp.float32),
            pltpu.VMEM((chunks * columns, slices), jnp.float32),
            pltpu.VMEM((chunks * pixels, slices), jnp.float32),
            pltpu.VMEM((angles * hit_rows, pixels), half),
            pltpu.VMEM((4, side, side), half),
            pltpu.VMEM((chunks, angles, hit_rows, slices), half),
            [pltpu.VMEM(((angles + 1) * detector - hit_rows, slices), half)] * chunks,
            pltpu.VMEM((chunks, angles, hit_rows, slices), half),
            pltpu.VMEM((chunks, angles, hit_rows, slices), half),
            pltpu.VMEM((chunks, columns, slices), half),
            pltpu.VMEM((strips, chunks, columns, slices), half),
        ] + [pltpu.VMEM((chunks, strips, columns, slices), half)] * 2 + [
            pltpu.VMEM((chunks, detector, slices), half),
            pltpu.VMEM((chunks, strips, detector, slices), half),
            [pltpu.VMEM((columns, slices), kind) for kind in wide_kinds],
            [pltpu.VMEM((strips, columns, slices), kind) for kind in wide_kinds],
            [pltpu.VMEM((detector, slices), half)] * chunks,
            pltpu.VMEM((chunks, detector, slices), jnp.float32),
            pltpu.VMEM((chunks, pad_rows, slices), jnp.float32),
            pltpu.VMEM((chunks, columns, slices), jnp.float32),
            pltpu.VMEM((chunks, columns, slices), jnp.float32),
            pltpu.VMEM((chunks, detector, slices), jnp.float32),
            pltpu.VMEM((pixels, angles * hit_rows), half),
            pltpu.SemaphoreType.DMA((9,)),
        ] + [pltpu.SemaphoreType.DMA((chunks,))] * 4
        + [pltpu.SemaphoreType.DMA((1 + 3 * chunks,))] * 2,
        compiler_params=pltpu.CompilerParams(
            collective_id=0, has_side_effects=True, vmem_limit_bytes=VMEM_BYTES
        ),
    )(
        positions.reshape(frames),
        tile_range.reshape(angles),
        measured[0],
        probe_field,
        object_field.reshape(chunks * columns, slices),
        dual_field.reshape(chunks * columns, slices),
        volume.reshape(chunks * pixels, slices),
        radon_tiles.reshape(angles * hit_rows, pixels),
        jnp.asarray(dft_tables(side)),
    )
    outs = pl.pallas_call(
        finish,
        out_shape=[jax.ShapeDtypeStruct(o.shape, o.dtype) for o in outs],
        in_specs=[pl.BlockSpec(memory_space=pl.ANY)] * 3,
        out_specs=[pl.BlockSpec(memory_space=pl.ANY)] * 3,
        scratch_shapes=[pltpu.SemaphoreType.DMA((3,))],
        compiler_params=pltpu.CompilerParams(vmem_limit_bytes=2 * 1024 * 1024),
    )(*outs)
    return (
        outs[0].reshape(object_field.shape),
        outs[1].reshape(dual_field.shape),
        outs[2].reshape(volume.shape),
    )


def solution(mesh):
    return jax.shard_map(
        body,
        mesh=mesh,
        in_specs=(
            P("ang", "strip", None, None),
            P("ang", "strip"),
            P(),
            P("ang", "strip", None, None),
            P("ang", "strip", None, None),
            P(("ang", "strip"), None, None),
            P(("ang", "strip"), None, None, None, None),
            P("ang", None, "strip", None),
        ),
        out_specs=(
            P("ang", "strip", None, None),
            P("ang", "strip", None, None),
            P(("ang", "strip"), None, None),
        ),
        check_vma=False,
    )
```

```python
import functools
import math

import jax
import jax.numpy as jnp
import numpy as np
from jax import lax
from jax.experimental import pallas as pl
from jax.experimental.pallas import tpu as pltpu
from jax.sharding import PartitionSpec as P

RAYS = 32
BLOCK = 128
VMEM_BYTES = 67043328 - 2 * 1024 * 1024

penalty = 1.0
object_step = 0.1
volume_step = 1.0
MESH = pl.DeviceIdType.MESH


def dft_tables(length):
    indices = np.arange(length, dtype=np.int64)
    angles = (indices[:, None] * indices[None, :] % length) * (2.0 * math.pi / length)
    scaling = 1.0 / math.sqrt(length)
    parts = []
    for table in (np.cos(angles) * scaling, np.sin(angles) * scaling):
        table = table.astype(np.float32)
        high = table.astype(jnp.bfloat16)
        parts += [high, (table - high.astype(np.float32)).astype(jnp.bfloat16)]
    return np.stack(parts)


def split(value):
    high = value.astype(jnp.bfloat16)
    return high, (value - high.astype(jnp.float32)).astype(jnp.bfloat16)


def dot(left, right):
    return jnp.dot(left, right, preferred_element_type=jnp.float32)


def dot3(left, right):
    return dot(
        jnp.concatenate([left[0], left[0], left[1]], axis=1),
        jnp.concatenate([right[0], right[1], right[0]], axis=0),
    )


def dot2(left, right):
    return dot(jnp.concatenate([left[0], left[1]], axis=1), jnp.concatenate([right, right], axis=0))


def beside(left, right):
    return jnp.concatenate([left, right], axis=1)


def above(top, low):
    return jnp.concatenate([top, low], axis=0)


def swap_blocks(value):
    half = value.shape[1] // 2
    return above(
        beside(value[:half, :half], value[half:, :half]),
        beside(value[:half, half:], value[half:, half:]),
    )


def both_parts(ref, columns):
    return beside(ref[pl.ds(0, columns, stride=2), :], ref[pl.ds(1, columns, stride=2), :])


def xor(left, right, bound):
    result, bit = 0, 1
    while bit < bound:
        result = result + ((left // bit) + (right // bit)) % 2 * bit
        bit *= 2
    return result


def kernel(
    angles, strips,
    positions_hbm, ranges_hbm, measured_hbm, probe_hbm, field_hbm, dual_hbm, volume_hbm, radon_hbm,
    tables_hbm,
    object_next, dual_next, volume_next,
    positions, ranges, measured, probe, field, dual, volume, radon, tables,
    ray_out, ray_in, pick_out, pick_in, field_out, field_in, grad_out, grad_in,
    mixed_out, mixed_in, wide_out, wide_in, rows_half, whole_field, grads,
    own_grad, own_rays, own_mixed, turned_radon,
    load_sem, ray_send, ray_recv, pick_send, pick_recv, strip_send, strip_recv,
):
    me, strip = lax.axis_index("ang"), lax.axis_index("strip")
    half_rows = radon.shape[0] // 2
    far_half = (me // (angles // 2) + 1) % 2
    far_rows = pl.ds(pl.multiple_of(far_half * half_rows, half_rows), half_rows)
    near_rows = pl.ds(pl.multiple_of((1 - far_half) * half_rows, half_rows), half_rows)
    loads = {}
    for k, (name, source, target) in enumerate((
        ("field", field_hbm, field), ("volume", volume_hbm, volume),
        ("radon_far", radon_hbm.at[far_rows], radon.at[far_rows]),
        ("radon_near", radon_hbm.at[near_rows], radon.at[near_rows]),
        ("dual", dual_hbm, dual), ("positions", positions_hbm, positions), ("ranges", ranges_hbm, ranges),
        ("tables", tables_hbm, tables), ("probe", probe_hbm, probe),
        ("measured", measured_hbm, measured),
    )):
        loads[name] = pltpu.make_async_copy(source, target, load_sem.at[k])
        loads[name].start()
    columns = field.shape[0] // 2
    detector = strips * columns
    frames, side = measured.shape[0], measured.shape[1]
    slices = field.shape[1]
    chunks, hit_rows = ray_out.shape[0], ray_out.shape[2]
    gap = detector - side
    if angles & (angles - 1) or angles < 4:
        groups, members, edge = 1, angles, me >= 0
        ang_peers = [lax.rem(me + offset, angles) for offset in range(1, angles)]
        far_peers = []
    else:
        groups, members, quarter = 2, angles // 2, angles // 4
        plane, low = me // quarter, lax.rem(me, quarter)
        side_of = me // members
        edge = (plane + 1) // 2 * 2 != 2
        mates = [xor(low, j, quarter) for j in range(quarter - 1, -1, -1)]
        ang_peers = [
            there * quarter + mate
            for there in (3 - 3 * side_of, 2 - side_of, 4 * side_of + 1 - plane)
            for mate in mates
        ] + [plane * quarter + mate for mate in mates[:-1]]
        far_peers = ang_peers[:members]
    near_peers = ang_peers[len(far_peers):]
    strip_peers = [lax.rem(strip + offset, strips) for offset in range(1, strips)]

    def rows_of(owner):
        return pl.ds(pl.multiple_of(owner * columns, columns), columns)

    barrier = pltpu.get_barrier_semaphore()
    for peer in ang_peers:
        pl.semaphore_signal(barrier, inc=1, device_id=(peer, strip), device_id_type=MESH)
    for peer in strip_peers:
        pl.semaphore_signal(barrier, inc=1, device_id=(me, peer), device_id_type=MESH)

    def remote(source, target, send, recv, device):
        return pltpu.make_async_remote_copy(
            src_ref=source, dst_ref=target, send_sem=send, recv_sem=recv,
            device_id=device, device_id_type=MESH,
        )

    others = pl.ds(0, angles - 1)
    slack = detector - hit_rows

    def window(slot):
        return pl.ds(pl.multiple_of(slack + slot * detector, RAYS), hit_rows)

    rest = pl.ds(0, strips - 1)

    def ray_copy(c, peer):
        return remote(
            ray_out.at[c, peer], ray_in[c].at[window(me)], ray_send.at[c], ray_recv.at[c],
            (peer, strip),
        )

    def ray_all(c):
        part = ray_in[c].at[pl.ds(0, (angles - 1) * hit_rows)]
        return remote(part, part, ray_send.at[c], ray_recv.at[c], (me, strip))

    def pick_copy(c, peer):
        return remote(
            pick_out.at[c, peer], pick_in.at[c, me], pick_send.at[c], pick_recv.at[c],
            (peer, strip),
        )

    def pick_all(c):
        return remote(
            pick_out.at[c, others], pick_in.at[c, others], pick_send.at[c], pick_recv.at[c],
            (me, strip),
        )

    def strip_copy(source, target, stage, peer):
        return remote(source, target, strip_send.at[stage], strip_recv.at[stage], (me, peer))

    def field_copy(peer):
        return strip_copy(field_out, field_in.at[strip], 0, peer)

    def grad_copy(c, peer):
        return strip_copy(grad_out.at[c, peer], grad_in.at[c, strip], 1 + c, peer)

    def wide_copy(c, peer):
        return strip_copy(wide_out[c], wide_in[c].at[strip], 1 + chunks + c, peer)

    def mixed_copy(c, owner, peer):
        return strip_copy(
            mixed_out.at[c, rows_of(owner), :], mixed_in.at[c, strip, rows_of(owner), :],
            1 + 2 * chunks + c, peer,
        )

    def strip_all(ref, stage):
        return strip_copy(ref.at[rest], ref.at[rest], stage, strip)

    loads["field"].wait()
    for c in range(chunks):
        own = field[pl.ds(c, columns, stride=chunks), :]
        field_out[c] = own.astype(jnp.bfloat16)
        whole_field[c, rows_of(strip), :] = own
    loads["volume"].wait()
    pixels = volume.shape[0] // 2
    volume_half = both_parts(volume, pixels).astype(jnp.bfloat16)
    loads["radon_far"].wait()
    if angles & (angles - 1) or angles < 4:
        loads["radon_near"].wait()
    def project(group):
        first = pl.multiple_of(group * members * hit_rows, hit_rows)
        sums = dot(radon[pl.ds(first, members * hit_rows), :], volume_half).astype(jnp.bfloat16)
        for c in range(chunks):
            ray_out[c, pl.ds(group * members, members)] = (
                sums[:, c * slices:(c + 1) * slices].reshape(members, hit_rows, slices)
            )

    def start_rays(c, peers):
        for peer in peers:
            ray_copy(c, peer).start()

    mine = me // members
    project(lax.rem(mine + groups - 1, groups))
    pl.semaphore_wait(barrier, len(ang_peers) + len(strip_peers))
    for peer in strip_peers:
        field_copy(peer).start()
    start_rays(0, far_peers)
    if groups > 1:
        loads["radon_near"].wait()
        project(mine)
    start_rays(0, near_peers)
    loads["dual"].wait()
    ray_weight = penalty - penalty * penalty * object_step
    grad_weight = penalty * object_step
    dual_weight = 1.0 - penalty * object_step
    for c in range(chunks):
        part = pl.ds(c, columns, stride=chunks)
        below = field[part, :] - field_out[c].astype(jnp.float32)
        wide_out[c][...] = (dual_weight * dual[part, :] + ray_weight * below).astype(
            wide_out[c].dtype
        )
    for c in range(chunks):
        for peer in strip_peers:
            wide_copy(c, peer).start()

    for c in range(chunks):
        for p in range(angles + 1):
            ray_in[c][pl.ds(p * detector, slack), :] = jnp.zeros((slack, slices), jnp.bfloat16)
        ray_in[c][window(me), :] = ray_out[c, me]
        for j in range(frames + 1):
            grads[c, pl.ds(j * (gap + side), gap), :] = jnp.zeros((gap, slices), jnp.float32)
    turned_radon[...] = radon[...].T
    for name in ("positions", "ranges", "tables", "probe", "measured"):
        loads[name].wait()
    cos_high, cos_low, sin_high, sin_low = (tables[k] for k in range(4))
    turn = tuple(
        above(beside(c, -s), beside(s, c)) for c, s in ((cos_high, sin_high), (cos_low, sin_low))
    )
    back_turn = tuple(
        above(beside(c, s), beside(-s, c)) for c, s in ((cos_high, sin_high), (cos_low, sin_low))
    )
    probe_re, probe_im = probe[0], probe[1]
    strip_all(field_in, 0).wait_recv()
    for peer in strip_peers:
        for c in range(chunks):
            whole_field[c, rows_of(peer), :] = field_in[peer, c].astype(jnp.float32)

    def frame_pair(pair):
        waves = []
        for j in (pair, pair + 1):
            re = whole_field[0, pl.ds(positions[j], side), :]
            im = whole_field[1, pl.ds(positions[j], side), :]
            waves.append(beside(probe_re * re - probe_im * im, probe_re * im + probe_im * re))
        right = dot3(split(above(*waves)), turn)
        far = dot3(back_turn, split(swap_blocks(right)))
        far_re, far_im = far[:side], far[side:]
        modulus = jnp.sqrt(far_re * far_re + far_im * far_im)
        intensity = beside(measured[pair], measured[pair + 1])
        shrink = 1.0 - jnp.sqrt(intensity) / jnp.maximum(modulus, 1.0)
        left = dot2(turn, above(far_re * shrink, far_im * shrink).astype(jnp.bfloat16))
        back = dot(
            beside(*[swap_blocks(left).astype(jnp.bfloat16)] * 2), above(*back_turn)
        )
        for k in range(2):
            part = back[k * side:(k + 1) * side]
            re, im = part[:, :side], part[:, side:]
            rows = pl.ds(gap + (pair + k) * (gap + side), side)
            grads[0, rows, :] = probe_re * re + probe_im * im
            grads[1, rows, :] = probe_re * im - probe_im * re

    def deposit(c, first, rows):
        total = None
        for j in range(frames):
            start = gap + j * (gap + side) + first - positions[j]
            piece = grads[c, pl.ds(start, rows), :]
            total = piece if total is None else total + piece
        return total

    def sum_rays(c, first, rows):
        total = None
        for p in range(angles):
            start = ((slack + p * detector + first) // RAYS - ranges[p]) * RAYS
            piece = ray_in[c][pl.ds(start, rows), :].astype(jnp.float32)
            total = piece if total is None else total + piece
        return total

    tiles, block = columns // RAYS, math.gcd(BLOCK, columns)

    def tile_rows(k):
        return pl.ds(k * RAYS, RAYS)

    def send_mixed(c):
        ray_all(c).wait_recv()
        for owner in [*strip_peers, strip]:
            for k in range(0, columns, block):
                first = pl.multiple_of(owner * columns + k, block)
                rays = sum_rays(c, first, block)
                grad = deposit(c, first, block)
                mixed = ray_weight * rays + grad_weight * grad
                own_mixed[c, pl.ds(first, block), :] = mixed
                mixed_out[c, pl.ds(first, block), :] = mixed.astype(jnp.bfloat16)
                if owner is strip:
                    own_rays[c, pl.ds(k, block), :] = rays
                    own_grad[c, pl.ds(k, block), :] = grad
                else:
                    grad_out[c, owner, pl.ds(k, block), :] = grad.astype(jnp.bfloat16)
            for peer in strip_peers:
                mixed_copy(c, owner, peer).start()

    def make_residual(c):
        strip_all(wide_in[c], 1 + chunks + c).wait_recv()
        strip_all(mixed_in.at[c], 1 + 2 * chunks + c).wait_recv()
        for owner in [*strip_peers, strip]:
            for k in range(tiles):
                rows = pl.ds(pl.multiple_of(owner * columns + k * RAYS, RAYS), RAYS)
                residual = own_mixed[c, rows, :] - ray_weight * whole_field[c, rows, :]
                if owner is strip:
                    part = pl.ds(c + k * RAYS * chunks, RAYS, stride=chunks)
                    residual = residual - dual_weight * dual[part, :]
                else:
                    residual = residual - wide_in[c][owner, tile_rows(k), :].astype(jnp.float32)
                for peer in strip_peers:
                    residual = residual + mixed_in[c, peer, rows, :].astype(jnp.float32)
                rows_half[c][rows, :] = residual.astype(jnp.bfloat16)

    def send_parts(c):
        for peer in strip_peers:
            grad_copy(c, peer).start()

    def update(c):
        strip_all(grad_in.at[c], 1 + c).wait_recv()
        for k in range(tiles):
            here = tile_rows(k)
            own_tile = pl.ds(pl.multiple_of(strip * columns + k * RAYS, RAYS), RAYS)
            intersection, projection = own_grad[c, here, :], own_rays[c, here, :]
            for peer in strip_peers:
                grad = grad_in[c, peer, here, :].astype(jnp.float32)
                mixed = mixed_in[c, peer, own_tile, :].astype(jnp.float32)
                intersection = intersection + grad
                projection = projection + (mixed - grad_weight * grad) * (1.0 / ray_weight)
            part = pl.ds(c + k * RAYS * chunks, RAYS, stride=chunks)
            part_field, part_dual = field[part, :], dual[part, :]
            updated = part_field - object_step * (
                intersection + part_dual + penalty * (part_field - projection)
            )
            object_next[part, :] = updated
            dual_next[part, :] = part_dual + penalty * (updated - projection)

    def send_picks(c):
        make_residual(c)
        for peer in ang_peers:
            pick_out[c, peer] = rows_half[c][pl.ds(ranges[peer] * RAYS, hit_rows), :]
            pick_copy(c, peer).start()
        pick_in[c, me] = rows_half[c][pl.ds(ranges[me] * RAYS, hit_rows), :]

    for pair in range(0, frames, 2):
        frame_pair(pair)
        if pair == 0:
            for c in range(1, chunks):
                start_rays(c, ang_peers)

    for c in range(chunks):
        send_mixed(c)
        send_picks(c)
    for c in range(chunks):
        send_parts(c)
    for c in range(chunks):
        update(c)
    for c in range(chunks):
        pick_all(c).wait_recv()
        gradient = dot(turned_radon[...], pick_in[c].reshape(angles * hit_rows, slices))
        part = pl.ds(c, pixels, stride=chunks)
        volume_next[part, :] = volume[part, :] - volume_step * gradient
    for peer in strip_peers:
        field_copy(peer).wait_send()
    for c in range(chunks):
        ray_all(c).wait_send()
        pick_all(c).wait_send()
        strip_all(grad_out.at[c], 1 + c).wait_send()
        strip_all(mixed_in.at[c], 1 + 2 * chunks + c).wait_send()
        for peer in strip_peers:
            wide_copy(c, peer).wait_send()


def finish(first, second, third, first_out, second_out, third_out, sem):
    copies = [
        pltpu.make_async_copy(source, target, sem.at[k])
        for k, (source, target) in enumerate(
            ((first, first_out), (second, second_out), (third, third_out))
        )
    ]
    for copy in copies:
        copy.start()
    for copy in copies:
        copy.wait()


def body(
    measured, positions, probe_field, object_field, dual_field, volume, radon_tiles, tile_range
):
    angles, strips = lax.axis_size("ang"), lax.axis_size("strip")
    frames, side = measured.shape[1], measured.shape[2]
    columns = object_field.shape[1]
    hit_rows = radon_tiles.shape[2] * radon_tiles.shape[3]
    pixels = radon_tiles.shape[4]
    chunks, slices = object_field.shape[2], object_field.shape[3]
    detector = strips * columns
    pad_rows = detector - side + frames * detector
    half = jnp.bfloat16
    wide_kinds = [half] + [jnp.float32] * (chunks - 1)
    outs = pl.pallas_call(
        functools.partial(kernel, angles, strips),
        out_shape=(
            pltpu.VMEM((chunks * columns, slices), jnp.float32),
            pltpu.VMEM((chunks * columns, slices), jnp.float32),
            pltpu.VMEM((chunks * pixels, slices), jnp.float32),
        ),
        in_specs=[pl.BlockSpec(memory_space=pltpu.HBM)] * 9,
        out_specs=(pl.BlockSpec(memory_space=pltpu.VMEM),) * 3,
        scratch_shapes=[
            pltpu.SMEM((frames,), jnp.int32),
            pltpu.SMEM((angles,), jnp.int32),
            pltpu.VMEM((frames, side, side), jnp.float32),
            pltpu.VMEM((chunks, side, side), jnp.float32),
            pltpu.VMEM((chunks * columns, slices), jnp.float32),
            pltpu.VMEM((chunks * columns, slices), jnp.float32),
            pltpu.VMEM((chunks * pixels, slices), jnp.float32),
            pltpu.VMEM((angles * hit_rows, pixels), half),
            pltpu.VMEM((4, side, side), half),
            pltpu.VMEM((chunks, angles, hit_rows, slices), half),
            [pltpu.VMEM(((angles + 1) * detector - hit_rows, slices), half)] * chunks,
            pltpu.VMEM((chunks, angles, hit_rows, slices), half),
            pltpu.VMEM((chunks, angles, hit_rows, slices), half),
            pltpu.VMEM((chunks, columns, slices), half),
            pltpu.VMEM((strips, chunks, columns, slices), half),
        ] + [pltpu.VMEM((chunks, strips, columns, slices), half)] * 2 + [
            pltpu.VMEM((chunks, detector, slices), half),
            pltpu.VMEM((chunks, strips, detector, slices), half),
            [pltpu.VMEM((columns, slices), kind) for kind in wide_kinds],
            [pltpu.VMEM((strips, columns, slices), kind) for kind in wide_kinds],
            [pltpu.VMEM((detector, slices), half)] * chunks,
            pltpu.VMEM((chunks, detector, slices), jnp.float32),
            pltpu.VMEM((chunks, pad_rows, slices), jnp.float32),
            pltpu.VMEM((chunks, columns, slices), jnp.float32),
            pltpu.VMEM((chunks, columns, slices), jnp.float32),
            pltpu.VMEM((chunks, detector, slices), jnp.float32),
            pltpu.VMEM((pixels, angles * hit_rows), half),
            pltpu.SemaphoreType.DMA((10,)),
        ] + [pltpu.SemaphoreType.DMA((chunks,))] * 4
        + [pltpu.SemaphoreType.DMA((1 + 3 * chunks,))] * 2,
        compiler_params=pltpu.CompilerParams(
            collective_id=0, has_side_effects=True, vmem_limit_bytes=VMEM_BYTES
        ),
    )(
        positions.reshape(frames),
        tile_range.reshape(angles),
        measured[0],
        probe_field,
        object_field.reshape(chunks * columns, slices),
        dual_field.reshape(chunks * columns, slices),
        volume.reshape(chunks * pixels, slices),
        radon_tiles.reshape(angles * hit_rows, pixels),
        jnp.asarray(dft_tables(side)),
    )
    outs = pl.pallas_call(
        finish,
        out_shape=[jax.ShapeDtypeStruct(o.shape, o.dtype) for o in outs],
        in_specs=[pl.BlockSpec(memory_space=pl.ANY)] * 3,
        out_specs=[pl.BlockSpec(memory_space=pl.ANY)] * 3,
        scratch_shapes=[pltpu.SemaphoreType.DMA((3,))],
        compiler_params=pltpu.CompilerParams(vmem_limit_bytes=2 * 1024 * 1024),
    )(*outs)
    return (
        outs[0].reshape(object_field.shape),
        outs[1].reshape(dual_field.shape),
        outs[2].reshape(volume.shape),
    )


def solution(mesh):
    return jax.shard_map(
        body,
        mesh=mesh,
        in_specs=(
            P("ang", "strip", None, None),
            P("ang", "strip"),
            P(),
            P("ang", "strip", None, None),
            P("ang", "strip", None, None),
            P(("ang", "strip"), None, None),
            P(("ang", "strip"), None, None, None, None),
            P("ang", None, "strip", None),
        ),
        out_specs=(
            P("ang", "strip", None, None),
            P("ang", "strip", None, None),
            P(("ang", "strip"), None, None),
        ),
        check_vma=False,
    )
```

```python
import functools
import math

import jax
import jax.numpy as jnp
import numpy as np
from jax import lax
from jax.experimental import pallas as pl
from jax.experimental.pallas import tpu as pltpu
from jax.sharding import PartitionSpec as P

RAYS = 32
BLOCK = 128
VMEM_BYTES = 67043328 - 2 * 1024 * 1024

penalty = 1.0
object_step = 0.1
volume_step = 1.0
MESH = pl.DeviceIdType.MESH


def dft_tables(length):
    indices = np.arange(length, dtype=np.int64)
    angles = (indices[:, None] * indices[None, :] % length) * (2.0 * math.pi / length)
    scaling = 1.0 / math.sqrt(length)
    parts = []
    for table in (np.cos(angles) * scaling, np.sin(angles) * scaling):
        table = table.astype(np.float32)
        high = table.astype(jnp.bfloat16)
        parts += [high, (table - high.astype(np.float32)).astype(jnp.bfloat16)]
    return np.stack(parts)


def split(value):
    high = value.astype(jnp.bfloat16)
    return high, (value - high.astype(jnp.float32)).astype(jnp.bfloat16)


def dot(left, right):
    return jnp.dot(left, right, preferred_element_type=jnp.float32)


def dot3(left, right):
    return dot(
        jnp.concatenate([left[0], left[0], left[1]], axis=1),
        jnp.concatenate([right[0], right[1], right[0]], axis=0),
    )


def dot2(left, right):
    return dot(jnp.concatenate([left[0], left[1]], axis=1), jnp.concatenate([right, right], axis=0))


def beside(left, right):
    return jnp.concatenate([left, right], axis=1)


def above(top, low):
    return jnp.concatenate([top, low], axis=0)


def swap_blocks(value):
    half = value.shape[1] // 2
    return above(
        beside(value[:half, :half], value[half:, :half]),
        beside(value[:half, half:], value[half:, half:]),
    )


def both_parts(ref, columns):
    return beside(ref[pl.ds(0, columns, stride=2), :], ref[pl.ds(1, columns, stride=2), :])


def xor(left, right, bound):
    result, bit = 0, 1
    while bit < bound:
        result = result + ((left // bit) + (right // bit)) % 2 * bit
        bit *= 2
    return result


def kernel(
    angles, strips,
    positions_hbm, ranges_hbm, measured_hbm, probe_hbm, field_hbm, dual_hbm, volume_hbm, radon_hbm,
    tables_hbm,
    object_next, dual_next, volume_next,
    positions, ranges, measured, probe, field, dual, volume, radon, tables,
    ray_out, ray_in, pick_out, pick_in, field_out, field_in, grad_out, grad_in,
    mixed_out, mixed_in, wide_out, wide_in, rows_half, whole_field, grads,
    own_grad, own_rays, own_mixed, turned_radon,
    load_sem, ray_send, ray_recv, pick_send, pick_recv, strip_send, strip_recv,
):
    loads = {}
    for k, (name, source, target) in enumerate((
        ("field", field_hbm, field), ("volume", volume_hbm, volume), ("radon", radon_hbm, radon),
        ("dual", dual_hbm, dual), ("positions", positions_hbm, positions), ("ranges", ranges_hbm, ranges),
        ("tables", tables_hbm, tables), ("probe", probe_hbm, probe),
        ("measured", measured_hbm, measured),
    )):
        loads[name] = pltpu.make_async_copy(source, target, load_sem.at[k])
        loads[name].start()
    me, strip = lax.axis_index("ang"), lax.axis_index("strip")
    columns = field.shape[0] // 2
    detector = strips * columns
    frames, side = measured.shape[0], measured.shape[1]
    slices = field.shape[1]
    chunks, hit_rows = ray_out.shape[0], ray_out.shape[2]
    gap = detector - side
    if angles & (angles - 1) or angles < 4:
        groups, members, edge = 1, angles, me >= 0
        ang_peers = [lax.rem(me + offset, angles) for offset in range(1, angles)]
        far_peers = []
    else:
        groups, members, quarter = 2, angles // 2, angles // 4
        plane, low = me // quarter, lax.rem(me, quarter)
        side_of = me // members
        edge = (plane + 1) // 2 * 2 != 2
        mates = [xor(low, j, quarter) for j in range(quarter - 1, -1, -1)]
        ang_peers = [
            there * quarter + mate
            for there in (3 - 3 * side_of, 2 - side_of, 4 * side_of + 1 - plane)
            for mate in mates
        ] + [plane * quarter + mate for mate in mates[:-1]]
        far_peers = ang_peers[:members]
    near_peers = ang_peers[len(far_peers):]
    strip_peers = [lax.rem(strip + offset, strips) for offset in range(1, strips)]

    def rows_of(owner):
        return pl.ds(pl.multiple_of(owner * columns, columns), columns)

    barrier = pltpu.get_barrier_semaphore()
    for peer in ang_peers:
        pl.semaphore_signal(barrier, inc=1, device_id=(peer, strip), device_id_type=MESH)
    for peer in strip_peers:
        pl.semaphore_signal(barrier, inc=1, device_id=(me, peer), device_id_type=MESH)

    def remote(source, target, send, recv, device):
        return pltpu.make_async_remote_copy(
            src_ref=source, dst_ref=target, send_sem=send, recv_sem=recv,
            device_id=device, device_id_type=MESH,
        )

    others = pl.ds(0, angles - 1)
    slack = detector - hit_rows

    def window(slot):
        return pl.ds(pl.multiple_of(slack + slot * detector, RAYS), hit_rows)

    rest = pl.ds(0, strips - 1)

    def ray_copy(c, peer):
        return remote(
            ray_out.at[c, peer], ray_in[c].at[window(me)], ray_send.at[c], ray_recv.at[c],
            (peer, strip),
        )

    def ray_all(c):
        part = ray_in[c].at[pl.ds(0, (angles - 1) * hit_rows)]
        return remote(part, part, ray_send.at[c], ray_recv.at[c], (me, strip))

    def pick_copy(c, peer, far):
        lane = c if far else chunks + c
        return remote(
            pick_out.at[c, peer], pick_in.at[c, me], pick_send.at[lane], pick_recv.at[lane],
            (peer, strip),
        )

    def pick_all(c, far):
        lane = c if far else chunks + c
        part = pl.ds(0, len(far_peers) if far else len(near_peers))
        return remote(
            pick_out.at[c, part], pick_in.at[c, part], pick_send.at[lane], pick_recv.at[lane],
            (me, strip),
        )

    def strip_copy(source, target, stage, peer):
        return remote(source, target, strip_send.at[stage], strip_recv.at[stage], (me, peer))

    def field_copy(peer):
        return strip_copy(field_out, field_in.at[strip], 0, peer)

    def grad_copy(c, peer):
        return strip_copy(grad_out.at[c, peer], grad_in.at[c, strip], 1 + c, peer)

    def wide_copy(c, peer):
        return strip_copy(wide_out[c], wide_in[c].at[strip], 1 + chunks + c, peer)

    def mixed_copy(c, owner, peer):
        return strip_copy(
            mixed_out.at[c, rows_of(owner), :], mixed_in.at[c, strip, rows_of(owner), :],
            1 + 2 * chunks + c, peer,
        )

    def strip_all(ref, stage):
        return strip_copy(ref.at[rest], ref.at[rest], stage, strip)

    loads["field"].wait()
    for c in range(chunks):
        own = field[pl.ds(c, columns, stride=chunks), :]
        field_out[c] = own.astype(jnp.bfloat16)
        whole_field[c, rows_of(strip), :] = own
    loads["volume"].wait()
    pixels = volume.shape[0] // 2
    volume_half = both_parts(volume, pixels).astype(jnp.bfloat16)
    loads["radon"].wait()
    def project(group):
        first = pl.multiple_of(group * members * hit_rows, hit_rows)
        sums = dot(radon[pl.ds(first, members * hit_rows), :], volume_half).astype(jnp.bfloat16)
        for c in range(chunks):
            ray_out[c, pl.ds(group * members, members)] = (
                sums[:, c * slices:(c + 1) * slices].reshape(members, hit_rows, slices)
            )

    def start_rays(c, peers):
        for peer in peers:
            ray_copy(c, peer).start()

    mine = me // members
    project(lax.rem(mine + groups - 1, groups))
    pl.semaphore_wait(barrier, len(ang_peers) + len(strip_peers))
    for peer in strip_peers:
        field_copy(peer).start()
    start_rays(0, far_peers)
    if groups > 1:
        project(mine)
    start_rays(0, near_peers)
    loads["dual"].wait()
    ray_weight = penalty - penalty * penalty * object_step
    grad_weight = penalty * object_step
    dual_weight = 1.0 - penalty * object_step
    for c in range(chunks):
        part = pl.ds(c, columns, stride=chunks)
        below = field[part, :] - field_out[c].astype(jnp.float32)
        wide_out[c][...] = (dual_weight * dual[part, :] + ray_weight * below).astype(
            wide_out[c].dtype
        )
    for c in range(chunks):
        for peer in strip_peers:
            wide_copy(c, peer).start()

    @pl.when(jnp.logical_not(edge))
    def _():
        for c in range(1, chunks):
            start_rays(c, ang_peers)

    for c in range(chunks):
        for p in range(angles + 1):
            ray_in[c][pl.ds(p * detector, slack), :] = jnp.zeros((slack, slices), jnp.bfloat16)
        ray_in[c][window(me), :] = ray_out[c, me]
        for j in range(frames + 1):
            grads[c, pl.ds(j * (gap + side), gap), :] = jnp.zeros((gap, slices), jnp.float32)
    turned_radon[...] = radon[...].T
    for name in ("positions", "ranges", "tables", "probe", "measured"):
        loads[name].wait()
    cos_high, cos_low, sin_high, sin_low = (tables[k] for k in range(4))
    turn = tuple(
        above(beside(c, -s), beside(s, c)) for c, s in ((cos_high, sin_high), (cos_low, sin_low))
    )
    back_turn = tuple(
        above(beside(c, s), beside(-s, c)) for c, s in ((cos_high, sin_high), (cos_low, sin_low))
    )
    probe_re, probe_im = probe[0], probe[1]
    strip_all(field_in, 0).wait_recv()
    for peer in strip_peers:
        for c in range(chunks):
            whole_field[c, rows_of(peer), :] = field_in[peer, c].astype(jnp.float32)

    def frame_pair(pair):
        waves = []
        for j in (pair, pair + 1):
            re = whole_field[0, pl.ds(positions[j], side), :]
            im = whole_field[1, pl.ds(positions[j], side), :]
            waves.append(beside(probe_re * re - probe_im * im, probe_re * im + probe_im * re))
        right = dot3(split(above(*waves)), turn)
        far = dot3(back_turn, split(swap_blocks(right)))
        far_re, far_im = far[:side], far[side:]
        modulus = jnp.sqrt(far_re * far_re + far_im * far_im)
        intensity = beside(measured[pair], measured[pair + 1])
        shrink = 1.0 - jnp.sqrt(intensity) / jnp.maximum(modulus, 1.0)
        left = dot2(turn, above(far_re * shrink, far_im * shrink).astype(jnp.bfloat16))
        back = dot(
            beside(*[swap_blocks(left).astype(jnp.bfloat16)] * 2), above(*back_turn)
        )
        for k in range(2):
            part = back[k * side:(k + 1) * side]
            re, im = part[:, :side], part[:, side:]
            rows = pl.ds(gap + (pair + k) * (gap + side), side)
            grads[0, rows, :] = probe_re * re + probe_im * im
            grads[1, rows, :] = probe_re * im - probe_im * re

    def deposit(c, first, rows):
        total = None
        for j in range(frames):
            start = gap + j * (gap + side) + first - positions[j]
            piece = grads[c, pl.ds(start, rows), :]
            total = piece if total is None else total + piece
        return total

    def sum_rays(c, first, rows):
        total = None
        for p in range(angles):
            start = ((slack + p * detector + first) // RAYS - ranges[p]) * RAYS
            piece = ray_in[c][pl.ds(start, rows), :].astype(jnp.float32)
            total = piece if total is None else total + piece
        return total

    tiles, block = columns // RAYS, math.gcd(BLOCK, columns)

    def tile_rows(k):
        return pl.ds(k * RAYS, RAYS)

    def send_mixed(c):
        ray_all(c).wait_recv()
        for owner in [*strip_peers, strip]:
            for k in range(0, columns, block):
                first = pl.multiple_of(owner * columns + k, block)
                rays = sum_rays(c, first, block)
                grad = deposit(c, first, block)
                mixed = ray_weight * rays + grad_weight * grad
                own_mixed[c, pl.ds(first, block), :] = mixed
                mixed_out[c, pl.ds(first, block), :] = mixed.astype(jnp.bfloat16)
                if owner is strip:
                    own_rays[c, pl.ds(k, block), :] = rays
                    own_grad[c, pl.ds(k, block), :] = grad
                else:
                    grad_out[c, owner, pl.ds(k, block), :] = grad.astype(jnp.bfloat16)
            for peer in strip_peers:
                mixed_copy(c, owner, peer).start()

    def make_residual(c):
        strip_all(wide_in[c], 1 + chunks + c).wait_recv()
        strip_all(mixed_in.at[c], 1 + 2 * chunks + c).wait_recv()
        for owner in [*strip_peers, strip]:
            for k in range(tiles):
                rows = pl.ds(pl.multiple_of(owner * columns + k * RAYS, RAYS), RAYS)
                residual = own_mixed[c, rows, :] - ray_weight * whole_field[c, rows, :]
                if owner is strip:
                    part = pl.ds(c + k * RAYS * chunks, RAYS, stride=chunks)
                    residual = residual - dual_weight * dual[part, :]
                else:
                    residual = residual - wide_in[c][owner, tile_rows(k), :].astype(jnp.float32)
                for peer in strip_peers:
                    residual = residual + mixed_in[c, peer, rows, :].astype(jnp.float32)
                rows_half[c][rows, :] = residual.astype(jnp.bfloat16)

    def send_parts(c):
        for peer in strip_peers:
            grad_copy(c, peer).start()

    def update(c):
        strip_all(grad_in.at[c], 1 + c).wait_recv()
        for k in range(tiles):
            here = tile_rows(k)
            own_tile = pl.ds(pl.multiple_of(strip * columns + k * RAYS, RAYS), RAYS)
            intersection, projection = own_grad[c, here, :], own_rays[c, here, :]
            for peer in strip_peers:
                grad = grad_in[c, peer, here, :].astype(jnp.float32)
                mixed = mixed_in[c, peer, own_tile, :].astype(jnp.float32)
                intersection = intersection + grad
                projection = projection + (mixed - grad_weight * grad) * (1.0 / ray_weight)
            part = pl.ds(c + k * RAYS * chunks, RAYS, stride=chunks)
            part_field, part_dual = field[part, :], dual[part, :]
            updated = part_field - object_step * (
                intersection + part_dual + penalty * (part_field - projection)
            )
            object_next[part, :] = updated
            dual_next[part, :] = part_dual + penalty * (updated - projection)

    def send_picks(c):
        make_residual(c)
        for far, peers in ((True, far_peers), (False, near_peers)):
            for peer in peers:
                pick_out[c, peer] = rows_half[c][pl.ds(ranges[peer] * RAYS, hit_rows), :]
                pick_copy(c, peer, far).start()
        pick_in[c, me] = rows_half[c][pl.ds(ranges[me] * RAYS, hit_rows), :]

    for pair in range(0, frames, 2):
        frame_pair(pair)
        if pair == 0:

            @pl.when(edge)
            def _():
                for c in range(1, chunks):
                    start_rays(c, ang_peers)

    for c in range(chunks):
        send_mixed(c)
        send_picks(c)
    for c in range(chunks):
        send_parts(c)
    for c in range(chunks):
        update(c)
    def part_gradient(c, group):
        rows = pick_in[c, pl.ds(group * members, members)].reshape(members * hit_rows, slices)
        first = pl.multiple_of(group * members * hit_rows, members * hit_rows)
        return dot(turned_radon[:, pl.ds(first, members * hit_rows)], rows)

    for c in range(chunks):
        part = pl.ds(c, pixels, stride=chunks)
        pick_all(c, False).wait_recv()
        volume_next[part, :] = volume[part, :] - volume_step * part_gradient(c, mine)
        if far_peers:
            pick_all(c, True).wait_recv()
            volume_next[part, :] = volume_next[part, :] - volume_step * part_gradient(
                c, 1 - mine
            )
    for peer in strip_peers:
        field_copy(peer).wait_send()
    for c in range(chunks):
        ray_all(c).wait_send()
        pick_all(c, False).wait_send()
        if far_peers:
            pick_all(c, True).wait_send()
        strip_all(grad_out.at[c], 1 + c).wait_send()
        strip_all(mixed_in.at[c], 1 + 2 * chunks + c).wait_send()
        for peer in strip_peers:
            wide_copy(c, peer).wait_send()


def finish(first, second, third, first_out, second_out, third_out, sem):
    copies = [
        pltpu.make_async_copy(source, target, sem.at[k])
        for k, (source, target) in enumerate(
            ((first, first_out), (second, second_out), (third, third_out))
        )
    ]
    for copy in copies:
        copy.start()
    for copy in copies:
        copy.wait()


def body(
    measured, positions, probe_field, object_field, dual_field, volume, radon_tiles, tile_range
):
    angles, strips = lax.axis_size("ang"), lax.axis_size("strip")
    frames, side = measured.shape[1], measured.shape[2]
    columns = object_field.shape[1]
    hit_rows = radon_tiles.shape[2] * radon_tiles.shape[3]
    pixels = radon_tiles.shape[4]
    chunks, slices = object_field.shape[2], object_field.shape[3]
    detector = strips * columns
    pad_rows = detector - side + frames * detector
    half = jnp.bfloat16
    wide_kinds = [half] + [jnp.float32] * (chunks - 1)
    outs = pl.pallas_call(
        functools.partial(kernel, angles, strips),
        out_shape=(
            pltpu.VMEM((chunks * columns, slices), jnp.float32),
            pltpu.VMEM((chunks * columns, slices), jnp.float32),
            pltpu.VMEM((chunks * pixels, slices), jnp.float32),
        ),
        in_specs=[pl.BlockSpec(memory_space=pltpu.HBM)] * 9,
        out_specs=(pl.BlockSpec(memory_space=pltpu.VMEM),) * 3,
        scratch_shapes=[
            pltpu.SMEM((frames,), jnp.int32),
            pltpu.SMEM((angles,), jnp.int32),
            pltpu.VMEM((frames, side, side), jnp.float32),
            pltpu.VMEM((chunks, side, side), jnp.float32),
            pltpu.VMEM((chunks * columns, slices), jnp.float32),
            pltpu.VMEM((chunks * columns, slices), jnp.float32),
            pltpu.VMEM((chunks * pixels, slices), jnp.float32),
            pltpu.VMEM((angles * hit_rows, pixels), half),
            pltpu.VMEM((4, side, side), half),
            pltpu.VMEM((chunks, angles, hit_rows, slices), half),
            [pltpu.VMEM(((angles + 1) * detector - hit_rows, slices), half)] * chunks,
            pltpu.VMEM((chunks, angles, hit_rows, slices), half),
            pltpu.VMEM((chunks, angles, hit_rows, slices), half),
            pltpu.VMEM((chunks, columns, slices), half),
            pltpu.VMEM((strips, chunks, columns, slices), half),
        ] + [pltpu.VMEM((chunks, strips, columns, slices), half)] * 2 + [
            pltpu.VMEM((chunks, detector, slices), half),
            pltpu.VMEM((chunks, strips, detector, slices), half),
            [pltpu.VMEM((columns, slices), kind) for kind in wide_kinds],
            [pltpu.VMEM((strips, columns, slices), kind) for kind in wide_kinds],
            [pltpu.VMEM((detector, slices), half)] * chunks,
            pltpu.VMEM((chunks, detector, slices), jnp.float32),
            pltpu.VMEM((chunks, pad_rows, slices), jnp.float32),
            pltpu.VMEM((chunks, columns, slices), jnp.float32),
            pltpu.VMEM((chunks, columns, slices), jnp.float32),
            pltpu.VMEM((chunks, detector, slices), jnp.float32),
            pltpu.VMEM((pixels, angles * hit_rows), half),
            pltpu.SemaphoreType.DMA((9,)),
        ] + [pltpu.SemaphoreType.DMA((chunks,))] * 2
        + [pltpu.SemaphoreType.DMA((2 * chunks,))] * 2
        + [pltpu.SemaphoreType.DMA((1 + 3 * chunks,))] * 2,
        compiler_params=pltpu.CompilerParams(
            collective_id=0, has_side_effects=True, vmem_limit_bytes=VMEM_BYTES
        ),
    )(
        positions.reshape(frames),
        tile_range.reshape(angles),
        measured[0],
        probe_field,
        object_field.reshape(chunks * columns, slices),
        dual_field.reshape(chunks * columns, slices),
        volume.reshape(chunks * pixels, slices),
        radon_tiles.reshape(angles * hit_rows, pixels),
        jnp.asarray(dft_tables(side)),
    )
    outs = pl.pallas_call(
        finish,
        out_shape=[jax.ShapeDtypeStruct(o.shape, o.dtype) for o in outs],
        in_specs=[pl.BlockSpec(memory_space=pl.ANY)] * 3,
        out_specs=[pl.BlockSpec(memory_space=pl.ANY)] * 3,
        scratch_shapes=[pltpu.SemaphoreType.DMA((3,))],
        compiler_params=pltpu.CompilerParams(vmem_limit_bytes=2 * 1024 * 1024),
    )(*outs)
    return (
        outs[0].reshape(object_field.shape),
        outs[1].reshape(dual_field.shape),
        outs[2].reshape(volume.shape),
    )


def solution(mesh):
    return jax.shard_map(
        body,
        mesh=mesh,
        in_specs=(
            P("ang", "strip", None, None),
            P("ang", "strip"),
            P(),
            P("ang", "strip", None, None),
            P("ang", "strip", None, None),
            P(("ang", "strip"), None, None),
            P(("ang", "strip"), None, None, None, None),
            P("ang", None, "strip", None),
        ),
        out_specs=(
            P("ang", "strip", None, None),
            P("ang", "strip", None, None),
            P(("ang", "strip"), None, None),
        ),
        check_vma=False,
    )
```
